32 devices in a mesh: lat: 4 (over z), lon: 8 (over y, x, core).
Axes of the slice: x: 2, y: 2, z: 4, core: 2. Of those that a mesh axis runs over, the one named last changes fastest.
Arguments:
- zonal_wind: float32 [32, 32, 2048], P(None, 'lat', 'lon'), may hold values from -6 to 6
- merid_wind: float32 [32, 32, 2048], P(None, 'lat', 'lon'), may hold values from -6 to 6
- vertical_wind: float32 [32, 32, 2048], P(None, 'lat', 'lon'), may hold values from -6 to 6
- pressure: float32 [32, 32, 2048], P(None, 'lat', 'lon'), may hold values from -6 to 6
- zonal_coef: float32 [32], P('lat'), may hold values from 0.05 to 0.4
- merid_coef: float32 [32], P('lat'), may hold values from 0.05 to 0.4
- level_coef: float32 [32], replicated, may hold values from 0.3 to 1.5
- sound_coef: float32 [32, 32, 2048], P(None, 'lat', 'lon'), may hold values from 0.2 to 2
- cutoff: int32 [32], replicated, may hold values from 1 to 511
- filter_mask: int32 [32], replicated, may hold values from 0 to 1, as said below
Outputs:
- zonal_next: float32 [32, 32, 2048], P(None, 'lat', 'lon')
- merid_next: float32 [32, 32, 2048], P(None, 'lat', 'lon')
- vertical_next: float32 [32, 32, 2048], P(None, 'lat', 'lon')
- pressure_next: float32 [32, 32, 2048], P(None, 'lat', 'lon')
The draws below stay inside these ranges and needn't reach their ends.
Inputs may be any that keep to these rules, and one draw needn't show every extreme that they name: `filter_mask`: for every latitude j below 16 exactly one of j and j + 16 is filtered; the filtered ones are the first n and the last 16 - n latitudes, for some n from 4 to 12.
All inputs are finite; a program needn't handle non-finite values.
Results may differ from the reference program's by a relative error of at most 0.0001.
Values sent between devices are 32-bit elements; how exact they have to be, the bound alone decides.
No kernel may reach another device: no remote copies, remote signals or barrier semaphores. Data moves between devices by JAX's collectives and lax.ppermute only.
A program may use at most 64 MiB of HBM per device.

```python
import math
import jax
import jax.numpy as jnp
from jax import lax

NLON = 2048
NLEV = 32
SUBSTEPS = 2
NLAT = 32


def draw_filter_mask(key, part):
    latitudes = jnp.arange(NLAT)
    northern = jax.random.randint(jax.random.fold_in(key, 17), (), NLAT // 8, 3 * NLAT // 8 + 1)
    southern_start = NLAT // 2 + northern
    return jnp.logical_or(latitudes < northern, latitudes >= southern_start).astype(jnp.int32)


def set_ends(drawn, own_key, smallest, top_value):
    place = [jax.random.randint(jax.random.fold_in(own_key, axis), (), 0, length) for axis, length in enumerate(drawn.shape)]
    widest = drawn.shape.index(max(drawn.shape))
    beside = place[:widest] + [(place[widest] + 1) % drawn.shape[widest]] + place[widest + 1:]
    return drawn.at[tuple(place)].set(smallest).at[tuple(beside)].set(top_value)


def block_scale(stream_key, extent, cuts, low, top_value):
    level = 1.0
    for position, parts in cuts:
        draws = jax.random.uniform(jax.random.fold_in(jax.random.fold_in(stream_key, 6), position), (parts,), jnp.float32, low / len(cuts), top_value / len(cuts))
        level = level * jnp.repeat(jnp.exp(draws), extent[position] // parts).reshape((-1,) + (1,) * (len(extent) - 1 - position))
    return level


def noise(own_key, dims, deviation, reach, shards=(), dtype=jnp.bfloat16):
    entries = deviation * jax.random.normal(own_key, dims, jnp.float32)
    if shards:
        entries = entries * block_scale(own_key, dims, shards, -0.22, 0.18)
    return jnp.clip(entries, -reach, reach).astype(dtype)


def setup_inputs(seed: int = 0) -> dict:
    streams_of = jax.random.split(jax.random.key(seed), 11)
    return {
        "zonal_wind": noise(streams_of[0], (NLEV, NLAT, NLON), 1.0, 6.0, ((1, 4), (2, 8)), jnp.float32),
        "merid_wind": noise(streams_of[1], (NLEV, NLAT, NLON), 1.0, 6.0, ((1, 4), (2, 8)), jnp.float32),
        "vertical_wind": noise(streams_of[2], (NLEV, NLAT, NLON), 1.0, 6.0, ((1, 4), (2, 8)), jnp.float32),
        "pressure": noise(streams_of[3], (NLEV, NLAT, NLON), 1.0, 6.0, ((1, 4), (2, 8)), jnp.float32),
        "zonal_coef": jnp.clip(jnp.exp(math.log(0.4) - 2.0794415 * jax.random.uniform(streams_of[4], (NLAT,), jnp.float32) ** block_scale(streams_of[4], (NLAT,), ((0, 4),), -0.2, 0.2)), 0.05, 0.4),
        "merid_coef": jnp.clip(jnp.exp(math.log(0.4) - 2.0794415 * jax.random.uniform(streams_of[5], (NLAT,), jnp.float32) ** block_scale(streams_of[5], (NLAT,), ((0, 4),), -0.2, 0.2)), 0.05, 0.4),
        "level_coef": jnp.clip(jnp.exp(jax.random.uniform(streams_of[6], (NLEV,), jnp.float32, math.log(0.3), math.log(1.5))), 0.3, 1.5),
        "sound_coef": jnp.clip(jnp.exp(math.log(2.0) - 2.3025851 * jax.random.uniform(streams_of[7], (NLEV, NLAT, NLON), jnp.float32) ** block_scale(streams_of[7], (NLEV, NLAT, NLON), ((1, 4), (2, 8)), -0.2, 0.2)), 0.2, 2.0),
        "cutoff": set_ends(jax.random.randint(streams_of[8], (NLAT,), 1, NLON // 4), jax.random.fold_in(streams_of[8], 1), 1, (NLON // 4) - 1).astype(jnp.int32),
        "filter_mask": draw_filter_mask(jax.random.fold_in(streams_of[10], 71), 0),
    }


def zonal_diff(field):
    return jnp.roll(field, -1, axis=2) - jnp.roll(field, 1, axis=2)


def merid_diff(field):
    padded = jnp.pad(field, ((0, 0), (1, 1), (0, 0)))
    return padded[:, 2:, :] - padded[:, :-2, :]


def damping(wavenum, limits):
    bound_col = limits[:, None]
    ratio = bound_col / jnp.maximum(wavenum[None, :], 1.0)
    return jnp.where(wavenum[None, :] > bound_col, ratio * ratio, 1.0)


def polar_damp(field, cutoff, filter_mask):
    wavenum = jnp.arange(NLON // 2 + 1).astype(jnp.float32)
    factor = damping(wavenum, cutoff.astype(jnp.float32))

    def one_level(slab):
        spectra = jnp.fft.rfft(slab, axis=1)
        return jnp.fft.irfft(spectra * factor, n=NLON, axis=1).astype(jnp.float32)

    damped = lax.map(one_level, field)
    return jnp.where(filter_mask[None, :, None] > 0, damped, field)


def column_solve(vertical_wind, pstar, level_coef, sound_coef):
    levels = vertical_wind.shape[0]
    zero_slab = jnp.zeros_like(vertical_wind[0])
    ratios = []
    values = []
    prev_ratio = zero_slab
    prev_value = zero_slab
    for level in range(levels):
        alpha = level_coef[level]
        below = alpha * sound_coef[level]
        if level + 1 < levels:
            above = alpha * sound_coef[level + 1]
            rhs = vertical_wind[level] - alpha * (pstar[level + 1] - pstar[level])
        else:
            above = zero_slab
            rhs = vertical_wind[level] + alpha * pstar[level]
        pivot = 1.0 + below + above + below * prev_ratio
        prev_ratio = -above / pivot
        prev_value = (rhs + below * prev_value) / pivot
        ratios.append(prev_ratio)
        values.append(prev_value)
    solved = [zero_slab] * levels
    upper_value = values[levels - 1]
    solved[levels - 1] = upper_value
    for level in range(levels - 2, -1, -1):
        upper_value = values[level] - ratios[level] * upper_value
        solved[level] = upper_value
    new_wind = jnp.stack(solved)
    wind_below = jnp.concatenate([zero_slab[None], new_wind[:-1]], axis=0)
    new_pressure = pstar - sound_coef * (new_wind - wind_below)
    return new_wind, new_pressure


def reference(zonal_wind, merid_wind, vertical_wind, pressure, zonal_coef, merid_coef, level_coef, sound_coef, cutoff, filter_mask):
    zonal_rows = zonal_coef[None, :, None]
    merid_rows = merid_coef[None, :, None]
    for step in range(SUBSTEPS):
        zonal_step = -zonal_rows * zonal_diff(pressure)
        merid_step = -merid_rows * merid_diff(pressure)
        zonal_wind = zonal_wind + polar_damp(zonal_step, cutoff, filter_mask)
        merid_wind = merid_wind + polar_damp(merid_step, cutoff, filter_mask)
        diverge = zonal_rows * zonal_diff(zonal_wind) + merid_rows * merid_diff(merid_wind)
        pstar = pressure - sound_coef * diverge
        vertical_wind, pressure = column_solve(vertical_wind, pstar, level_coef, sound_coef)
    return (zonal_wind, merid_wind, vertical_wind, pressure)
```

```python
import functools
import math

import jax
import jax.numpy as jnp
import numpy as np
from jax import lax
from jax.experimental import pallas as pl
from jax.experimental.pallas import tpu as pltpu
from jax.sharding import PartitionSpec as P

SUBSTEPS = 2
LANES = 128
F32 = jnp.float32
BF16 = jnp.bfloat16


def cmul_const(re, im, cr, ci):
    if im is None:
        return (re * cr if cr != 0.0 else None, re * ci if ci != 0.0 else None)
    return (re * cr - im * ci, re * ci + im * cr)


def add(a, b):
    if a is None:
        return b
    return a if b is None else a + b


def sub(a, b):
    if b is None:
        return a
    return -b if a is None else a - b


def neg(a):
    return None if a is None else -a


def unit(num, den):
    turn = num % den
    table = {0: (1.0, 0.0), den / 4: (0.0, 1.0), den / 2: (-1.0, 0.0), 3 * den / 4: (0.0, -1.0)}
    if turn in table:
        return table[turn]
    angle = 2.0 * math.pi * turn / den
    return math.cos(angle), math.sin(angle)


def rotate(z, num, den):
    cr, ci = unit(num, den)
    re, im = z
    if (cr, ci) == (1.0, 0.0):
        return z
    if (cr, ci) == (0.0, 1.0):
        return (neg(im), re)
    if (cr, ci) == (0.0, -1.0):
        return (im, neg(re))
    return cmul_const(re, im, cr, ci)


def real_dft(pieces):
    n = len(pieces)
    if n == 1:
        return [(pieces[0], None)]
    even, odd = real_dft(pieces[0::2]), real_dft(pieces[1::2])
    out = [None] * (n // 2 + 1)
    for s in range(n // 4 + 1 if n > 2 else 1):
        er, ei = even[s]
        tr, ti = rotate(odd[s], -s, n)
        out[n // 2 - s] = (sub(er, tr), sub(ti, ei))
        out[s] = (add(er, tr), add(ei, ti))
    return out


def real_dft_inverse(groups):
    n = 2 * (len(groups) - 1)
    if n == 0:
        return [groups[0][0]]
    if n == 2:
        a, b = groups[0][0], groups[1][0]
        return [a + b, a - b]
    even, odd = [], []
    for s in range(n // 4 + 1):
        ar, ai = groups[s]
        br, bi = groups[n // 2 - s]
        even.append((add(ar, br), sub(ai, bi)))
        odd.append(rotate((sub(ar, br), add(ai, bi)), s, n))
    if True:
        even[0] = (even[0][0], None)
        odd[0] = (odd[0][0], None)
        even[-1] = (even[-1][0], None)
        odd[-1] = (odd[-1][0], None)
    out = [None] * n
    out[0::2] = real_dft_inverse(even)
    out[1::2] = real_dft_inverse(odd)
    return out


def tables(length):
    pieces = length // LANES
    groups = pieces // 2 + 1
    lane = np.arange(LANES)
    angle = 2.0 * np.pi / LANES * (np.outer(lane, lane) % LANES)
    cos, sin = np.cos(angle), np.sin(angle)
    matrix = np.block([[cos, -sin], [sin, cos]])

    def halves(m):
        m = m.astype(np.float32)
        high = m.astype(BF16)
        return np.stack([high, (m - high.astype(np.float32)).astype(BF16)])

    weights = np.stack([halves(matrix), halves(matrix.T)])
    s = np.arange(groups)[:, None]
    turn = 2.0 * np.pi / length * (s * lane[None, :])
    wavenum = pieces * lane[None, :] + s
    wavenum = np.minimum(wavenum, length - wavenum).astype(np.float64)
    slope = 2.0 * np.sin(2.0 * np.pi / length * (pieces * lane[None, :] + s))
    rows = np.stack([np.cos(turn), np.sin(turn), wavenum, 1.0 / np.maximum(wavenum, 1.0) ** 2, slope])
    return weights, rows.astype(np.float32)


def transform_kernel(plan, full, x_ref, coef_ref, weight_ref, table_ref, *refs):
    outs, (lhs_ref, spec_ref, work_ref) = refs[:-3], refs[-3:]
    stacks, stack_step, nl, piece_step, skip, band = plan
    _, tall, width = x_ref.shape
    per = width // LANES
    pieces = nl * per
    groups = pieces // 2 + 1
    rows = stacks * tall
    length = pieces * LANES

    def block(stack, l):
        return stack * stack_step + l * piece_step

    def product(which, count):
        total = jnp.dot(lhs_ref[0, :count], weight_ref[which, 0], preferred_element_type=F32)
        total += jnp.dot(lhs_ref[1, :count], weight_ref[which, 0], preferred_element_type=F32)
        return total + jnp.dot(lhs_ref[0, :count], weight_ref[which, 1], preferred_element_type=F32)

    def put(row, re, im):
        for half, part in enumerate((re, im)):
            high = part.astype(BF16)
            low = (part - high.astype(F32)).astype(BF16)
            lhs_ref[0, row:row + rows, half * LANES:(half + 1) * LANES] = high
            lhs_ref[1, row:row + rows, half * LANES:(half + 1) * LANES] = low

    chunks = []
    for l in range(nl):
        for h in range(per):
            chunks.append(jnp.concatenate([x_ref[block(z, l), :, h * LANES:(h + 1) * LANES] for z in range(stacks)], axis=0))
    zero = jnp.zeros((rows, LANES), F32)
    for s, (re, im) in enumerate(real_dft(chunks)):
        if s:
            cr, ci = table_ref[0, s:s + 1], table_ref[1, s:s + 1]
            if im is None:
                re, im = re * cr, -re * ci
            else:
                re, im = re * cr + im * ci, im * cr - re * ci
        put(s * rows, re, zero if im is None else im)
    spec_ref[...] = product(0, groups * rows)

    limit, has_up, has_down, zonal2, merid, merid_up, merid_down = (coef_ref[i] for i in range(7))
    limit2 = limit * limit

    def above(a):
        return pltpu.roll(a, rows - 1, 0)

    def below(a):
        return pltpu.roll(a, 1, 0)

    for s in range(groups):
        wavenum, inverse2, slope = (table_ref[i, s:s + 1] for i in (2, 3, 4))
        factor = jnp.where(wavenum > limit, limit2 * inverse2, 1.0)
        parts = [spec_ref[s * rows:(s + 1) * rows, half * LANES:(half + 1) * LANES] for half in (0, 1)]
        zonal = zonal2 * (slope * slope)
        filtered = [factor * part for part in parts]
        merids, divs = [], []
        for part, filt in zip(parts, filtered):
            across = factor * (has_up * above(part) - has_down * below(part))
            flux = merid * across
            merids.append(across)
            divs.append(zonal * filt - merid_up * above(flux) + merid_down * below(flux))
        put(s * rows, *divs)
        if full:
            put((groups + s) * rows, -slope * filtered[1], slope * filtered[0])
            put((2 * groups + s) * rows, *merids)

    count = (3 if full else 1) * groups * rows
    work_ref[...] = product(1, count)
    for field in range(3 if full else 1):
        spectrum = []
        for s in range(groups):
            base = (field * groups + s) * rows
            re = work_ref[base:base + rows, :LANES]
            im = work_ref[base:base + rows, LANES:]
            if s:
                cr, ci = table_ref[0, s:s + 1], table_ref[1, s:s + 1]
                re, im = re * cr - im * ci, (None if s == groups - 1 else re * ci + im * cr)
            else:
                im = None
            spectrum.append((re, im))
        result = real_dft_inverse(spectrum)
        target, offset = (outs[0], 0) if field == 0 else (outs[1], (field - 1) * band)
        for l in range(nl):
            for h in range(per):
                piece = result[l * per + h] * (1.0 / length)
                for z in range(stacks):
                    first = z * tall + skip
                    target[block(z, l), offset:offset + band, h * LANES:(h + 1) * LANES] = piece[first:first + band]


def transform(x, coefs, weights, table, plan, full):
    blocks, tall, width = x.shape
    band = plan[5]
    rows = plan[0] * tall
    groups = table.shape[1]
    count = (3 if full else 1) * groups * rows
    shapes = [jax.ShapeDtypeStruct((blocks, band, width), F32)]
    if full:
        shapes.append(jax.ShapeDtypeStruct((blocks, 2 * band, width), F32))
    return pl.pallas_call(
        functools.partial(transform_kernel, plan, full),
        out_shape=shapes,
        scratch_shapes=[
            pltpu.VMEM((2, count, 2 * LANES), BF16),
            pltpu.VMEM((groups * rows, 2 * LANES), F32),
            pltpu.VMEM((count, 2 * LANES), F32),
        ],
        cost_estimate=pl.CostEstimate(flops=6 * 2 * 65536 * count, bytes_accessed=8 * x.size, transcendentals=0),
        name="transform_all" if full else "transform_div",
    )(x, coefs, weights, table)


def factor_kernel(level_ref, sound_ref, inv_ref, carry_ref, ratio_ref):
    levels = sound_ref.shape[0]
    prev = jnp.zeros(sound_ref.shape[1:], F32)
    for k in range(levels):
        alpha = level_ref[k]
        below = alpha * sound_ref[k]
        above = alpha * sound_ref[k + 1] if k + 1 < levels else jnp.zeros_like(below)
        inv = 1.0 / (1.0 + below + above + below * prev)
        prev = -above * inv
        inv_ref[k] = inv
        carry_ref[k] = below * inv
        ratio_ref[k] = prev


def factor(level_coef, sound):
    shape = jax.ShapeDtypeStruct(sound.shape, F32)
    return pl.pallas_call(
        factor_kernel,
        in_specs=[pl.BlockSpec(memory_space=pltpu.SMEM), pl.BlockSpec(memory_space=pltpu.VMEM)],
        out_shape=[shape] * 3,
        cost_estimate=pl.CostEstimate(flops=10 * sound.size, bytes_accessed=16 * sound.size, transcendentals=0),
        name="factor_columns",
    )(level_coef, sound)


def column_kernel(first, level_ref, sound_ref, inv_ref, carry_ref, ratio_ref, base_ref, div_ref, p_ref, w_ref, *outs):
    w_out, p_out = outs[0], outs[1]
    levels = sound_ref.shape[0]

    def star(k):
        return p_ref[k] - sound_ref[k] * (base_ref[k] + div_ref[k])

    here = star(0)
    value = None
    for k in range(levels):
        alpha = level_ref[k]
        p_out[k] = here
        if k + 1 < levels:
            upper = star(k + 1)
            rhs = w_ref[k] - alpha * (upper - here)
            here = upper
        else:
            rhs = w_ref[k] + alpha * here
        scaled = rhs * inv_ref[k]
        value = scaled if value is None else scaled + carry_ref[k] * value
        w_out[k] = value
    upper = w_out[levels - 1]
    for k in range(levels - 1, -1, -1):
        lower = w_out[k - 1] - ratio_ref[k - 1] * upper if k else None
        if k:
            w_out[k - 1] = lower
        fresh = p_out[k] - sound_ref[k] * (upper if lower is None else upper - lower)
        p_out[k] = fresh
        if first:
            outs[2][k] = p_ref[k] + fresh
        upper = lower


def column(level_coef, sound, factors, base, div, p, w, first):
    shape = jax.ShapeDtypeStruct(sound.shape, F32)
    return pl.pallas_call(
        functools.partial(column_kernel, first),
        in_specs=[pl.BlockSpec(memory_space=pltpu.SMEM)] + [pl.BlockSpec(memory_space=pltpu.VMEM)] * 8,
        out_shape=[shape] * (3 if first else 2),
        cost_estimate=pl.CostEstimate(flops=20 * sound.size, bytes_accessed=40 * sound.size, transcendentals=0),
        name="column_first" if first else "column_last",
    )(level_coef, sound, *factors, base, div, p, w)


def shifted(block, axis, step):
    count = lax.axis_size(axis)
    return lax.ppermute(block, axis, [(i, (i + step) % count) for i in range(count)])


def exchange(block, axes):
    return lax.all_to_all(block, axes, split_axis=0, concat_axis=0, tiled=True)


def lat_edges(last, first):
    count = lax.axis_size("lat")
    low = lax.ppermute(last, "lat", [(i, i + 1) for i in range(count - 1)])
    high = lax.ppermute(first, "lat", [(i + 1, i) for i in range(count - 1)])
    return low, high


def latitude_data(zonal_coef, merid_coef, merid_wind, halo):
    levels, band, width = merid_wind.shape
    nz, me = lax.axis_size("lat"), lax.axis_index("lat")
    if halo:
        v_low, v_high = lat_edges(merid_wind[:, -1], merid_wind[:, 0])
        own = jnp.stack([zonal_coef, merid_coef])
        low, high = lat_edges(own[:, -halo:], own[:, :halo])
        zonal, merid = jnp.concatenate([low, own, high], axis=1)
        return zonal, merid, v_low, v_high
    target = lax.broadcasted_iota(jnp.int32, (nz, 1, 1), 0)
    edges = jnp.where(target == me + 1, merid_wind[None, :, band - 1], 0.0)
    edges = jnp.where(target == me - 1, merid_wind[None, :, 0], edges)
    own = jnp.concatenate([zonal_coef, merid_coef])
    own = jnp.broadcast_to(jnp.pad(own, (0, width - 2 * band)), (nz, 8, width))
    sent = jnp.concatenate([edges, own], axis=1).reshape(nz * (levels + 8), width)
    got = exchange(sent, "lat").reshape(nz, levels + 8, width)
    padded = jnp.pad(got[:, :levels], ((1, 1), (0, 0), (0, 0)))
    v_low = lax.dynamic_index_in_dim(padded, me, 0, keepdims=False)
    v_high = lax.dynamic_index_in_dim(padded, me + 2, 0, keepdims=False)
    zonal = got[:, levels, :band].reshape(nz * band)
    merid = got[:, levels, band:2 * band].reshape(nz * band)
    return zonal, merid, v_low, v_high


def body(
    zonal_wind,
    merid_wind,
    vertical_wind,
    pressure,
    zonal_coef,
    merid_coef,
    level_coef,
    sound_coef,
    cutoff,
    filter_mask,
):
    levels, band, width = pressure.shape
    nz, nl = lax.axis_size("lat"), lax.axis_size("lon")
    length = width * nl
    lats = band * nz
    me = lax.axis_index("lat")
    both = ("lat", "lon")
    weights, table = tables(length)

    if levels % (nz * nl) == 0:
        axes, halo, tall = both, 0, band
        depth = levels // (nz * nl)
        plan = (nz * depth, 1, nl, depth, 0, band)
        if depth == 1:
            plan = (nz, nl, nl, 1, 0, band)
    else:
        axes, halo, tall = "lon", 2, -(-(band + 4) // 8) * 8
        depth = levels // nl
        plan = (depth, 1, nl, depth, 2, band)

    def spread(field):
        if halo:
            low, high = lat_edges(field[:, -halo:], field[:, :halo])
            field = jnp.concatenate([low, field, high], axis=1)
            field = jnp.pad(field, ((0, 0), (0, tall - band - 2 * halo), (0, 0)))
        return exchange(field, axes)

    circles = spread(pressure)

    zonal_all, merid_all, v_low, v_high = latitude_data(zonal_coef, merid_coef, merid_wind, halo)
    row = jnp.arange(lats + 2 * halo) - halo
    has_up = (row < lats - 1).astype(F32)
    has_down = (row > 0).astype(F32)
    limit = jnp.pad(jnp.where(filter_mask > 0, cutoff, length).astype(F32), (halo, halo), constant_values=1.0)
    coefs = jnp.stack([limit, has_up, has_down])
    if halo:
        coefs = lax.dynamic_slice_in_dim(coefs, me * band, band + 2 * halo, 1)
    coefs = jnp.concatenate([coefs, (zonal_all * zonal_all)[None], merid_all[None], merid_all * coefs[1:3]])
    if halo:
        coefs = jnp.tile(jnp.pad(coefs, ((0, 0), (0, tall - band - 2 * halo))), (1, depth))
    coefs = jnp.broadcast_to(coefs[:, :, None], coefs.shape + (LANES,))

    u_low = shifted(zonal_wind[:, :, -1:], "lon", 1)
    u_high = shifted(zonal_wind[:, :, :1], "lon", -1)
    zonal_rows, merid_rows = zonal_coef[None, :, None], merid_coef[None, :, None]
    u_diff = jnp.concatenate([zonal_wind[:, :, 1:], u_high], 2) - jnp.concatenate([u_low, zonal_wind[:, :, :-1]], 2)
    v_diff = jnp.concatenate([merid_wind[:, 1:], v_high[:, None]], 1) - jnp.concatenate([v_low[:, None], merid_wind[:, :-1]], 1)
    base = zonal_rows * u_diff + merid_rows * v_diff

    factors = factor(level_coef, sound_coef)

    (div,) = transform(circles, coefs, weights, table, plan, False)
    div = exchange(div, axes)
    w, p, total = column(level_coef, sound_coef, factors, base, div, pressure, vertical_wind, True)
    div, winds = transform(spread(total), coefs, weights, table, plan, True)
    div = exchange(div, axes)
    winds = exchange(winds, axes)
    w, p = column(level_coef, sound_coef, factors, base, div, p, w, False)
    u = zonal_wind - zonal_rows * winds[:, :band]
    v = merid_wind - merid_rows * winds[:, band:]
    return (u, v, w, p)


def solution(mesh):
    spec = P(None, "lat", "lon")
    in_specs = (spec, spec, spec, spec, P("lat"), P("lat"), P(), spec, P(), P())
    return jax.shard_map(body, mesh=mesh, in_specs=in_specs, out_specs=(spec,) * 4, check_vma=False)
```

```python
import functools
import math

import jax
import jax.numpy as jnp
import numpy as np
from jax import lax
from jax.experimental import pallas as pl
from jax.experimental.pallas import tpu as pltpu
from jax.sharding import PartitionSpec as P


LANES = 128
F32 = jnp.float32
BF16 = jnp.bfloat16
KERNEL = pltpu.CompilerParams(vmem_limit_bytes=8 << 20)


def cmul_const(re, im, cr, ci):
    if im is None:
        return (re * cr if cr != 0.0 else None, re * ci if ci != 0.0 else None)
    return (re * cr - im * ci, re * ci + im * cr)


def add(a, b):
    if a is None:
        return b
    return a if b is None else a + b


def sub(a, b):
    if b is None:
        return a
    return -b if a is None else a - b


def neg(a):
    return None if a is None else -a


def unit(num, den):
    turn = num % den
    table = {0: (1.0, 0.0), den / 4: (0.0, 1.0), den / 2: (-1.0, 0.0), 3 * den / 4: (0.0, -1.0)}
    if turn in table:
        return table[turn]
    angle = 2.0 * math.pi * turn / den
    return math.cos(angle), math.sin(angle)


def rotate(z, num, den):
    cr, ci = unit(num, den)
    re, im = z
    if (cr, ci) == (1.0, 0.0):
        return z
    if (cr, ci) == (0.0, 1.0):
        return (neg(im), re)
    if (cr, ci) == (0.0, -1.0):
        return (im, neg(re))
    return cmul_const(re, im, cr, ci)


def real_dft(pieces):
    n = len(pieces)
    if n == 1:
        return [(pieces[0], None)]
    even, odd = real_dft(pieces[0::2]), real_dft(pieces[1::2])
    out = [None] * (n // 2 + 1)
    for s in range(n // 4 + 1 if n > 2 else 1):
        er, ei = even[s]
        tr, ti = rotate(odd[s], -s, n)
        out[n // 2 - s] = (sub(er, tr), sub(ti, ei))
        out[s] = (add(er, tr), add(ei, ti))
    return out


def real_dft_inverse(groups):
    n = 2 * (len(groups) - 1)
    if n == 0:
        return [groups[0][0]]
    if n == 2:
        a, b = groups[0][0], groups[1][0]
        return [a + b, a - b]
    even, odd = [], []
    for s in range(n // 4 + 1):
        ar, ai = groups[s]
        br, bi = groups[n // 2 - s]
        even.append((add(ar, br), sub(ai, bi)))
        odd.append(rotate((sub(ar, br), add(ai, bi)), s, n))
    even[0] = (even[0][0], None)
    odd[0] = (odd[0][0], None)
    even[-1] = (even[-1][0], None)
    odd[-1] = (odd[-1][0], None)
    out = [None] * n
    out[0::2] = real_dft_inverse(even)
    out[1::2] = real_dft_inverse(odd)
    return out


def tables(length):
    pieces = length // LANES
    groups = pieces // 2 + 1
    lane = np.arange(LANES)
    angle = 2.0 * np.pi / LANES * (np.outer(lane, lane) % LANES)
    cos, sin = np.cos(angle), np.sin(angle)
    matrix = np.block([[cos, -sin], [sin, cos]])

    def halves(m):
        m = m.astype(np.float32)
        high = m.astype(BF16)
        return np.stack([high, (m - high.astype(np.float32)).astype(BF16)])

    weights = np.stack([halves(matrix), halves(matrix.T)])
    s = np.arange(groups)[:, None]
    turn = 2.0 * np.pi / length * (s * lane[None, :])
    wavenum = pieces * lane[None, :] + s
    wavenum = np.minimum(wavenum, length - wavenum).astype(np.float64)
    slope = 2.0 * np.sin(2.0 * np.pi / length * (pieces * lane[None, :] + s))
    rows = np.stack([np.cos(turn), np.sin(turn), wavenum, 1.0 / np.maximum(wavenum, 1.0) ** 2, slope])
    return weights, rows.astype(np.float32)


def transform_kernel(plan, full, x_ref, coef_ref, weight_ref, table_ref, out_ref, lhs_ref, spec_ref, work_ref):
    stacks, stack_step, nl, piece_step, skip, band = plan
    _, tall, width = x_ref.shape
    per = width // LANES
    pieces = nl * per
    groups = pieces // 2 + 1
    rows = stacks * tall
    length = pieces * LANES

    def block(stack, l):
        return stack * stack_step + l * piece_step

    def product(which, count):
        total = jnp.dot(lhs_ref[0, :count], weight_ref[which, 0], preferred_element_type=F32)
        total += jnp.dot(lhs_ref[1, :count], weight_ref[which, 0], preferred_element_type=F32)
        return total + jnp.dot(lhs_ref[0, :count], weight_ref[which, 1], preferred_element_type=F32)

    def put(row, re, im):
        for half, part in enumerate((re, im)):
            high = part.astype(BF16)
            low = (part - high.astype(F32)).astype(BF16)
            lhs_ref[0, row:row + rows, half * LANES:(half + 1) * LANES] = high
            lhs_ref[1, row:row + rows, half * LANES:(half + 1) * LANES] = low

    chunks = []
    for l in range(nl):
        for h in range(per):
            chunks.append(jnp.concatenate([x_ref[block(z, l), :, h * LANES:(h + 1) * LANES] for z in range(stacks)], axis=0))
    zero = jnp.zeros((rows, LANES), F32)
    for s, (re, im) in enumerate(real_dft(chunks)):
        if s:
            cr, ci = table_ref[0, s:s + 1], table_ref[1, s:s + 1]
            if im is None:
                re, im = re * cr, -re * ci
            else:
                re, im = re * cr + im * ci, im * cr - re * ci
        put(s * rows, re, zero if im is None else im)
    spec_ref[...] = product(0, groups * rows)

    limit, has_up, has_down, zonal, merid = (jnp.broadcast_to(coef_ref[:, i:i + 1], (rows, LANES)) for i in range(5))
    zonal2, merid_up, merid_down = zonal * zonal, merid * has_up, merid * has_down
    limit2 = limit * limit

    def above(a):
        return pltpu.roll(a, rows - 1, 0)

    def below(a):
        return pltpu.roll(a, 1, 0)

    for s in range(groups):
        wavenum, inverse2, slope = (table_ref[i, s:s + 1] for i in (2, 3, 4))
        factor = jnp.where(wavenum > limit, limit2 * inverse2, 1.0)
        parts = [spec_ref[s * rows:(s + 1) * rows, half * LANES:(half + 1) * LANES] for half in (0, 1)]
        spread2 = zonal2 * (slope * slope)
        filtered = [factor * part for part in parts]
        merids, divs = [], []
        for part, filt in zip(parts, filtered):
            across = factor * (has_up * above(part) - has_down * below(part))
            flux = merid * across
            merids.append(across)
            divs.append(spread2 * filt - merid_up * above(flux) + merid_down * below(flux))
        put(s * rows, *divs)
        if full:
            put((groups + s) * rows, -slope * filtered[1], slope * filtered[0])
            put((2 * groups + s) * rows, *merids)

    count = (3 if full else 1) * groups * rows
    work_ref[...] = product(1, count)
    for field in range(3 if full else 1):
        spectrum = []
        for s in range(groups):
            base = (field * groups + s) * rows
            re = work_ref[base:base + rows, :LANES]
            im = work_ref[base:base + rows, LANES:]
            if s:
                cr, ci = table_ref[0, s:s + 1], table_ref[1, s:s + 1]
                re, im = re * cr - im * ci, (None if s == groups - 1 else re * ci + im * cr)
            else:
                im = None
            spectrum.append((re, im))
        result = real_dft_inverse(spectrum)
        offset = field * band
        for l in range(nl):
            for h in range(per):
                piece = result[l * per + h] * (1.0 / length)
                for z in range(stacks):
                    first = z * tall + skip
                    out_ref[block(z, l), offset:offset + band, h * LANES:(h + 1) * LANES] = piece[first:first + band]


def transform(x, coefs, weights, table, plan, full):
    blocks, tall, width = x.shape
    band = plan[5]
    rows = plan[0] * tall
    groups = table.shape[1]
    fields = 3 if full else 1
    count = fields * groups * rows
    return pl.pallas_call(
        functools.partial(transform_kernel, plan, full),
        out_shape=jax.ShapeDtypeStruct((blocks, fields * band, width), F32),
        scratch_shapes=[
            pltpu.VMEM((2, count, 2 * LANES), BF16),
            pltpu.VMEM((groups * rows, 2 * LANES), F32),
            pltpu.VMEM((count, 2 * LANES), F32),
        ],
        compiler_params=KERNEL,
        cost_estimate=pl.CostEstimate(flops=6 * 2 * 65536 * count, bytes_accessed=8 * x.size, transcendentals=0),
        name="transform_all" if full else "transform_div",
    )(x, coefs, weights, table)


def factor_kernel(level_ref, sound_ref, inv_ref, carry_ref, ratio_ref):
    levels = sound_ref.shape[0]
    prev = jnp.zeros(sound_ref.shape[1:], F32)
    for k in range(levels):
        alpha = level_ref[k]
        below = alpha * sound_ref[k]
        above = alpha * sound_ref[k + 1] if k + 1 < levels else jnp.zeros_like(below)
        inv = 1.0 / (1.0 + below + above + below * prev)
        prev = -above * inv
        inv_ref[k] = inv
        carry_ref[k] = below * inv
        ratio_ref[k] = prev


def factor(level_coef, sound):
    shape = jax.ShapeDtypeStruct(sound.shape, F32)
    return pl.pallas_call(
        factor_kernel,
        in_specs=[pl.BlockSpec(memory_space=pltpu.SMEM), pl.BlockSpec(memory_space=pltpu.VMEM)],
        out_shape=[shape] * 3,
        compiler_params=KERNEL,
        cost_estimate=pl.CostEstimate(flops=10 * sound.size, bytes_accessed=16 * sound.size, transcendentals=0),
        name="factor_columns",
    )(level_coef, sound)


def column_kernel(first, level_ref, sound_ref, inv_ref, carry_ref, ratio_ref, base_ref, div_ref, p_ref, w_ref, *refs):
    if first:
        w_out, p_out, sum_out = refs
    else:
        u_ref, v_ref, rows_ref, u_out, v_out, w_out, p_out = refs
    levels, band, _ = sound_ref.shape

    def star(k):
        return p_ref[k] - sound_ref[k] * (base_ref[k] + div_ref[k, :band])

    here = star(0)
    value = None
    for k in range(levels):
        alpha = level_ref[k]
        p_out[k] = here
        if k + 1 < levels:
            upper = star(k + 1)
            rhs = w_ref[k] - alpha * (upper - here)
            here = upper
        else:
            rhs = w_ref[k] + alpha * here
        scaled = rhs * inv_ref[k]
        value = scaled if value is None else scaled + carry_ref[k] * value
        w_out[k] = value
        if not first:
            zonal, merid = rows_ref[:, 0:1], rows_ref[:, 1:2]
            u_out[k] = u_ref[k] - zonal * div_ref[k, band:2 * band]
            v_out[k] = v_ref[k] - merid * div_ref[k, 2 * band:]
    upper = w_out[levels - 1]
    for k in range(levels - 1, -1, -1):
        lower = w_out[k - 1] - ratio_ref[k - 1] * upper if k else None
        if k:
            w_out[k - 1] = lower
        fresh = p_out[k] - sound_ref[k] * (upper if lower is None else upper - lower)
        p_out[k] = fresh
        if first:
            sum_out[k] = p_ref[k] + fresh
        upper = lower


def column(first, level_coef, *operands):
    shape = jax.ShapeDtypeStruct(operands[0].shape, F32)
    size = operands[0].size
    return pl.pallas_call(
        functools.partial(column_kernel, first),
        in_specs=[pl.BlockSpec(memory_space=pltpu.SMEM)] + [pl.BlockSpec(memory_space=pltpu.VMEM)] * len(operands),
        out_shape=[shape] * (3 if first else 4),
        compiler_params=KERNEL,
        cost_estimate=pl.CostEstimate(flops=20 * size, bytes_accessed=40 * size, transcendentals=0),
        name="column_first" if first else "column_last",
    )(level_coef, *operands)


def shifted(block, axis, step):
    count = lax.axis_size(axis)
    return lax.ppermute(block, axis, [(i, (i + step) % count) for i in range(count)])


def exchange(block, axes):
    return lax.all_to_all(block, axes, split_axis=0, concat_axis=0, tiled=True)


def lat_edges(last, first):
    count = lax.axis_size("lat")
    low = lax.ppermute(last, "lat", [(i, i + 1) for i in range(count - 1)])
    high = lax.ppermute(first, "lat", [(i + 1, i) for i in range(count - 1)])
    return low, high


def latitude_data(coefs, halo):
    nz, me = lax.axis_size("lat"), lax.axis_index("lat")
    if halo:
        low, high = lat_edges(coefs[-halo:], coefs[:halo])
        return jnp.concatenate([low, coefs, high], axis=0)
    got = [coefs]
    for step in range(1, nz):
        got.append(lax.ppermute(coefs, "lat", [(i, (i + step) % nz) for i in range(nz)]))
    blocks = []
    for z in range(nz):
        block = got[0]
        for k in range(1, nz):
            block = jnp.where((me - z) % nz == k, got[k], block)
        blocks.append(block)
    return jnp.concatenate(blocks, axis=0)


def program(
    zonal_wind,
    merid_wind,
    vertical_wind,
    pressure,
    zonal_coef,
    merid_coef,
    level_coef,
    sound_coef,
    cutoff,
    filter_mask,
):
    levels, band, width = pressure.shape
    nz, nl = lax.axis_size("lat"), lax.axis_size("lon")
    length = width * nl
    lats = band * nz
    me = lax.axis_index("lat")
    both = ("lat", "lon")
    weights, table = tables(length)

    if levels % (nz * nl) == 0:
        axes, halo, tall = both, 0, band
        depth = levels // (nz * nl)
        plan = (nz * depth, 1, nl, depth, 0, band)
        if depth == 1:
            plan = (nz, nl, nl, 1, 0, band)
    else:
        axes, halo, tall = "lon", 2, -(-(band + 4) // 8) * 8
        depth = levels // nl
        plan = (depth, 1, nl, depth, 2, band)

    def spread(field):
        if halo:
            low, high = lat_edges(field[:, -halo:], field[:, :halo])
            field = jnp.concatenate([low, field, high], axis=1)
            field = jnp.pad(field, ((0, 0), (0, tall - band - 2 * halo), (0, 0)))
        return exchange(field, axes)

    circles = spread(pressure)

    row = jnp.arange(lats + 2 * halo) - halo
    limit = jnp.pad(jnp.where(filter_mask > 0, cutoff, length).astype(F32), (halo, halo), constant_values=1.0)
    known = jnp.stack([limit, (row < lats - 1).astype(F32), (row > 0).astype(F32)], axis=1)
    if halo:
        known = lax.dynamic_slice_in_dim(known, me * band, band + 2 * halo, 0)
    coefs = jnp.concatenate([known, latitude_data(jnp.stack([zonal_coef, merid_coef], axis=1), halo)], axis=1)
    if halo:
        coefs = jnp.tile(jnp.pad(coefs, ((0, tall - band - 2 * halo), (0, 0))), (depth, 1))

    v_low, v_high = lat_edges(merid_wind[:, -1:], merid_wind[:, :1])
    u_low = shifted(zonal_wind[:, :, -1:], "lon", 1)
    u_high = shifted(zonal_wind[:, :, :1], "lon", -1)
    zonal_rows, merid_rows = zonal_coef[None, :, None], merid_coef[None, :, None]
    u_diff = jnp.concatenate([zonal_wind[:, :, 1:], u_high], 2) - jnp.concatenate([u_low, zonal_wind[:, :, :-1]], 2)
    v_diff = jnp.concatenate([merid_wind[:, 1:], v_high], 1) - jnp.concatenate([v_low, merid_wind[:, :-1]], 1)
    base = zonal_rows * u_diff + merid_rows * v_diff

    factors = factor(level_coef, sound_coef)

    div = transform(circles, coefs, weights, table, plan, False)
    div = exchange(div, axes)
    w, p, total = column(True, level_coef, sound_coef, *factors, base, div, pressure, vertical_wind)
    fields = transform(spread(total), coefs, weights, table, plan, True)
    fields = exchange(fields, axes)
    rows = jnp.stack([zonal_coef, merid_coef], axis=1)
    return column(False, level_coef, sound_coef, *factors, base, fields, p, w, zonal_wind, merid_wind, rows)


def solution(mesh):
    spec = P(None, "lat", "lon")
    in_specs = (spec, spec, spec, spec, P("lat"), P("lat"), P(), spec, P(), P())
    return jax.shard_map(program, mesh=mesh, in_specs=in_specs, out_specs=(spec,) * 4, check_vma=False)
```

```python
import functools
import math
from typing import NamedTuple

import jax
import jax.numpy as jnp
import numpy as np
from jax import lax
from jax.experimental import pallas as pl
from jax.experimental.pallas import tpu as pltpu
from jax.sharding import PartitionSpec as P


LANES = 128
F32 = jnp.float32
BF16 = jnp.bfloat16
KERNEL = pltpu.CompilerParams(vmem_limit_bytes=8 << 20)
ALONE = pltpu.CompilerParams(vmem_limit_bytes=60 << 20)


class Plan(NamedTuple):
    packed: bool
    offsets: tuple
    depth: int
    nl: int
    per: int
    tall: int
    skip: int
    band: int

    def fields(self, full):
        if not full:
            return "d"
        return "uv" if self.packed else "duv"


def cmul_const(re, im, cr, ci):
    if im is None:
        return (re * cr if cr != 0.0 else None, re * ci if ci != 0.0 else None)
    return (re * cr - im * ci, re * ci + im * cr)


def add(a, b):
    if a is None:
        return b
    return a if b is None else a + b


def sub(a, b):
    if b is None:
        return a
    return -b if a is None else a - b


def neg(a):
    return None if a is None else -a


def unit(num, den):
    turn = num % den
    table = {0: (1.0, 0.0), den / 4: (0.0, 1.0), den / 2: (-1.0, 0.0), 3 * den / 4: (0.0, -1.0)}
    if turn in table:
        return table[turn]
    angle = 2.0 * math.pi * turn / den
    return math.cos(angle), math.sin(angle)


def rotate(z, num, den):
    cr, ci = unit(num, den)
    re, im = z
    if (cr, ci) == (1.0, 0.0):
        return z
    if (cr, ci) == (0.0, 1.0):
        return (neg(im), re)
    if (cr, ci) == (0.0, -1.0):
        return (im, neg(re))
    return cmul_const(re, im, cr, ci)


def real_dft(pieces):
    n = len(pieces)
    if n == 1:
        return [(pieces[0], None)]
    even, odd = real_dft(pieces[0::2]), real_dft(pieces[1::2])
    out = [None] * (n // 2 + 1)
    for s in range(n // 4 + 1 if n > 2 else 1):
        er, ei = even[s]
        tr, ti = rotate(odd[s], -s, n)
        out[n // 2 - s] = (sub(er, tr), sub(ti, ei))
        out[s] = (add(er, tr), add(ei, ti))
    return out


def real_dft_inverse(groups):
    n = 2 * (len(groups) - 1)
    if n == 0:
        return [groups[0][0]]
    if n == 2:
        a, b = groups[0][0], groups[1][0]
        return [a + b, a - b]
    even, odd = [], []
    for s in range(n // 4 + 1):
        ar, ai = groups[s]
        br, bi = groups[n // 2 - s]
        even.append((add(ar, br), sub(ai, bi)))
        odd.append(rotate((sub(ar, br), add(ai, bi)), s, n))
    even[0] = (even[0][0], None)
    odd[0] = (odd[0][0], None)
    even[-1] = (even[-1][0], None)
    odd[-1] = (odd[-1][0], None)
    out = [None] * n
    out[0::2] = real_dft_inverse(even)
    out[1::2] = real_dft_inverse(odd)
    return out


def tables(length):
    pieces = length // LANES
    groups = pieces // 2 + 1
    lane = np.arange(LANES)
    angle = 2.0 * np.pi / LANES * (np.outer(lane, lane) % LANES)
    cos, sin = np.cos(angle), np.sin(angle)
    matrix = np.block([[cos, -sin], [sin, cos]])

    def halves(m):
        m = m.astype(np.float32)
        high = m.astype(BF16)
        return np.stack([high, (m - high.astype(np.float32)).astype(BF16)])

    weights = np.stack([halves(matrix), halves(matrix.T)])
    s = np.arange(groups)[:, None]
    turn = 2.0 * np.pi / length * (s * lane[None, :])
    wavenum = pieces * lane[None, :] + s
    wavenum = np.minimum(wavenum, length - wavenum).astype(np.float64)
    slope = 2.0 * np.sin(2.0 * np.pi / length * (pieces * lane[None, :] + s))
    rows = np.stack([np.cos(turn), np.sin(turn), wavenum, 1.0 / np.maximum(wavenum, 1.0) ** 2, slope])
    return weights, rows.astype(np.float32)


def transform_kernel(plan, full, x_ref, *refs):
    extra_ref = x_ref
    if plan.packed and full:
        extra_ref, refs = refs[0], refs[1:]
    coef_ref, weight_ref, table_ref, result_ref, lhs_ref, spec_ref, work_ref, out_ref, sem = refs
    nl, per, tall, skip, band = plan.nl, plan.per, plan.tall, plan.skip, plan.band
    stacks = len(plan.offsets)
    pieces = nl * per
    groups = pieces // 2 + 1
    rows = stacks * tall
    length = pieces * LANES

    def block(stack, l):
        return plan.offsets[stack] + l % nl * plan.depth

    def tile(stack, l, h):
        return x_ref[block(stack, l), h * tall:(h + 1) * tall]

    def edge_tile(stack, l):
        return unfold(extra_ref[block(stack, l), per * tall + 4:per * tall + 8])

    def product(which, count):
        total = jnp.dot(lhs_ref[0, :count], weight_ref[which, 0], preferred_element_type=F32)
        total += jnp.dot(lhs_ref[1, :count], weight_ref[which, 0], preferred_element_type=F32)
        return total + jnp.dot(lhs_ref[0, :count], weight_ref[which, 1], preferred_element_type=F32)

    def put(row, re, im):
        for half, part in enumerate((re, im)):
            high = part.astype(BF16)
            low = (part - high.astype(F32)).astype(BF16)
            lhs_ref[0, row:row + rows, half * LANES:(half + 1) * LANES] = high
            lhs_ref[1, row:row + rows, half * LANES:(half + 1) * LANES] = low

    chunks = []
    for l in range(nl):
        for h in range(per):
            chunks.append(jnp.concatenate([tile(z, l, h) for z in range(stacks)], axis=0))
    zero = jnp.zeros((rows, LANES), F32)
    for s, (re, im) in enumerate(real_dft(chunks)):
        if s:
            cr, ci = table_ref[0, s:s + 1], table_ref[1, s:s + 1]
            if im is None:
                re, im = re * cr, -re * ci
            else:
                re, im = re * cr + im * ci, im * cr - re * ci
        put(s * rows, re, zero if im is None else im)
    spec_ref[...] = product(0, groups * rows)

    def column(a):
        return jnp.broadcast_to(a, (a.shape[0], LANES))

    if plan.packed:
        limit = column(coef_ref[...])
        place = lax.broadcasted_iota(jnp.int32, (rows, LANES), 0) % (2 * tall)
        has_up = jnp.where(place < 2 * tall - 1, 1.0, 0.0)
        has_down = jnp.where(place > 0, 1.0, 0.0)
        pair = [edge_tile(z, 0) for z in range(2)]
        zonal = jnp.concatenate([column(t[:, 1:2]) for t in pair] * (stacks // 2), axis=0)
        merid = jnp.concatenate([column(t[:, 2:3]) for t in pair] * (stacks // 2), axis=0)
    else:
        limit, has_up, has_down, zonal, merid = (column(coef_ref[:, i:i + 1]) for i in range(5))
    zonal2, merid_up, merid_down = zonal * zonal, merid * has_up, merid * has_down
    limit2 = limit * limit

    def above(a):
        return pltpu.roll(a, rows - 1, 0)

    def below(a):
        return pltpu.roll(a, 1, 0)

    for s in range(groups):
        wavenum, inverse2, slope = (table_ref[i, s:s + 1] for i in (2, 3, 4))
        factor = jnp.where(wavenum > limit, limit2 * inverse2, 1.0)
        parts = [spec_ref[s * rows:(s + 1) * rows, half * LANES:(half + 1) * LANES] for half in (0, 1)]
        spread2 = zonal2 * (slope * slope)
        filtered = [factor * part for part in parts]
        merids, divs = [], []
        for part, filt in zip(parts, filtered):
            across = factor * (has_up * above(part) - has_down * below(part))
            flux = merid * across
            merids.append(across)
            divs.append(spread2 * filt - merid_up * above(flux) + merid_down * below(flux))
        spectra = {"d": divs, "u": (-slope * filtered[1], slope * filtered[0]), "v": merids}
        for field, name in enumerate(plan.fields(full)):
            put((field * groups + s) * rows, *spectra[name])

    count = len(plan.fields(full)) * groups * rows
    work_ref[...] = product(1, count)
    results = []
    for field in range(len(plan.fields(full))):
        spectrum = []
        for s in range(groups):
            base = (field * groups + s) * rows
            re = work_ref[base:base + rows, :LANES]
            im = work_ref[base:base + rows, LANES:]
            if s:
                cr, ci = table_ref[0, s:s + 1], table_ref[1, s:s + 1]
                re, im = re * cr - im * ci, (None if s == groups - 1 else re * ci + im * cr)
            else:
                im = None
            spectrum.append((re, im))
        result = real_dft_inverse(spectrum)
        results.append([piece * (1.0 / length) for piece in result])

    row = lax.broadcasted_iota(jnp.int32, (band, LANES), 0)
    lane = lax.broadcasted_iota(jnp.int32, (band, LANES), 1)
    for z in range(stacks):
        first = z * tall + skip
        last = first + band
        own_zonal = zonal[first:last]
        if plan.packed:
            edges = [edge_tile(z, l) for l in range(nl)]
            spot = per * tall
            side = band - 1 if z % 2 == 0 else 0
            sign = 1.0 if z % 2 == 0 else -1.0
            v_weight = jnp.where(row == side, sign * merid[first:last], 0.0)
            west = jnp.where(lane == 0, -own_zonal, 0.0)
            east = jnp.where(lane == LANES - 1, own_zonal, 0.0)
        for l in range(nl):
            here = block(z, l)
            if plan.packed and full:
                for field in range(2):
                    for h in range(per):
                        at = (field * per + h) * band
                        out_ref[here, at:at + band] = results[field][l * per + h][first:last]
                u, v = results
                before = u[(l * per - 1) % pieces][first:last]
                after = u[(l * per + per) % pieces][first:last]
                before = edges[l - 1] - own_zonal * pltpu.roll(before, 1, 1)
                after = edges[(l + 1) % nl] - own_zonal * pltpu.roll(after, LANES - 1, 1)
                edge = jnp.where(lane == 0, before, jnp.where(lane == LANES - 1, after, 0.0))
                at = 2 * per * band
                out_ref[here, at + 4:at + 8] = fold(edge, row)
                other = (z ^ 1) * tall + (0 if z % 2 == 0 else band - 1)
                for h in range(per):
                    moved = merid[other:other + 1] * v[l * per + h][other:other + 1]
                    out_ref[here, at + h:at + h + 1] = extra_ref[block(z ^ 1, l), spot + h:spot + h + 1] - moved
                if per < 4:
                    out_ref[here, at + per:at + 4] = jnp.zeros((4 - per, LANES), F32)
                continue
            for field in range(len(results)):
                for h in range(per):
                    value = results[field][l * per + h][first:last]
                    if plan.packed:
                        value += v_weight * extra_ref[block(z ^ 1, l), spot + h:spot + h + 1]
                        if h == 0:
                            value += west * edges[l - 1]
                        if h == per - 1:
                            value += east * edges[(l + 1) % nl]
                    out_ref[here, field * band:(field + 1) * band, h * LANES:(h + 1) * LANES] = value
    leave = pltpu.make_async_copy(out_ref, result_ref, sem)
    leave.start()
    leave.wait()


def fold(edge, row):
    edge = jnp.where(row < 4, edge, pltpu.roll(edge, LANES // 2, 1))
    return edge[:4] + edge[4:]


def unfold(part):
    return jnp.concatenate([part, pltpu.roll(part, LANES // 2, 1)], axis=0)


def transform(plan, full, coefs, weights, table, *operands):
    rows = len(plan.offsets) * plan.tall
    fields = len(plan.fields(full))
    groups = table.shape[1]
    count = fields * groups * rows
    blocks, width = operands[0].shape[0], plan.per * LANES
    shape = (blocks, fields * plan.band, width)
    if plan.packed and full:
        shape = (blocks, (2 * plan.per + 1) * plan.band, LANES)
    return pl.pallas_call(
        functools.partial(transform_kernel, plan, full),
        out_specs=pl.BlockSpec(memory_space=pltpu.HBM),
        out_shape=jax.ShapeDtypeStruct(shape, F32),
        scratch_shapes=[
            pltpu.VMEM((2, count, 2 * LANES), BF16),
            pltpu.VMEM((groups * rows, 2 * LANES), F32),
            pltpu.VMEM((count, 2 * LANES), F32),
            pltpu.VMEM(shape, F32),
            pltpu.SemaphoreType.DMA,
        ],
        compiler_params=KERNEL,
        cost_estimate=pl.CostEstimate(flops=6 * 2 * 65536 * count, bytes_accessed=32 * blocks * plan.band * width, transcendentals=0),
        name="transform_all" if full else "transform_div",
    )(*operands, coefs, weights, table)


def pack_kernel(zonal_ref, merid_ref, p_ref, u_ref, v_ref, result_ref, rows_ref, out_ref, u_buf, v_buf, sems):
    levels, band, width = u_buf.shape
    per = width // LANES
    moves = [pltpu.make_async_copy(u_ref, u_buf, sems.at[0]), pltpu.make_async_copy(v_ref, v_buf, sems.at[1])]
    for h in range(per):
        source = p_ref.at[:, :, pl.ds(h * LANES, LANES)]
        moves.append(pltpu.make_async_copy(source, out_ref.at[:, pl.ds(h * band, band)], sems.at[2 + h]))
    for move in moves:
        move.start()
    odd = lax.axis_index("lat") % 2 == 1
    row = lax.broadcasted_iota(jnp.int32, (band, LANES), 0)
    lane = lax.broadcasted_iota(jnp.int32, (band, LANES), 1)
    coefs = jnp.zeros((band, LANES), F32)
    for j in range(band):
        coefs = jnp.where(row == j, jnp.where(lane == 1, zonal_ref[j], jnp.where(lane == 2, merid_ref[j], 0.0)), coefs)
    facing = jnp.where(odd, merid_ref[band - 1], merid_ref[0])
    blank = jnp.zeros((4 - per, LANES), F32)
    for move in moves:
        move.wait()
    for k in range(levels):
        west = pltpu.roll(u_buf[k, :, width - LANES:], 1, 1)
        east = pltpu.roll(u_buf[k, :, :LANES], LANES - 1, 1)
        edge = jnp.where(lane == 0, west, jnp.where(lane == LANES - 1, east, coefs))
        base = per * band
        out_ref[k, base + 4:base + 8] = fold(edge, row)
        for h in range(per):
            lanes = slice(h * LANES, (h + 1) * LANES)
            top, bottom = v_buf[k, :1, lanes], v_buf[k, band - 1:, lanes]
            out_ref[k, base + h:base + h + 1] = jnp.where(odd, top, bottom)
            rows_ref[k, 2:3, lanes] = jnp.where(odd, bottom, top)
            rows_ref[k, :2, lanes] = jnp.where(odd, out_ref[k, h * band + band - 2:h * band + band], out_ref[k, h * band:h * band + 2])
        rows_ref[k, 3:4] = jnp.full((1, width), facing, F32)
        if per < 4:
            out_ref[k, base + per:base + 4] = blank
    leave = pltpu.make_async_copy(out_ref, result_ref, sems.at[0])
    leave.start()
    leave.wait()


def pack(zonal, merid, p, u, v):
    levels, band, width = p.shape
    shape = (levels, (width // LANES + 1) * band, LANES)
    hbm = pl.BlockSpec(memory_space=pltpu.HBM)
    return pl.pallas_call(
        pack_kernel,
        in_specs=[pl.BlockSpec(memory_space=pltpu.SMEM)] * 2 + [hbm] * 3,
        out_specs=[hbm, pl.BlockSpec(memory_space=pltpu.VMEM)],
        out_shape=[jax.ShapeDtypeStruct(shape, F32), jax.ShapeDtypeStruct((levels, 4, width), F32)],
        scratch_shapes=[
            pltpu.VMEM(shape, F32),
            pltpu.VMEM(p.shape, F32),
            pltpu.VMEM(p.shape, F32),
            pltpu.SemaphoreType.DMA((2 + width // LANES,)),
        ],
        compiler_params=ALONE,
        cost_estimate=pl.CostEstimate(flops=p.size, bytes_accessed=16 * p.size, transcendentals=0),
        name="pack_circles",
    )(zonal, merid, p, u, v)


def factor_kernel(level_ref, sound_ref, *refs):
    if len(refs) > 1:
        u_ref, v_ref, own_ref, inv_ref, base_ref = refs
        band, width = u_ref.shape[1:]
        row = lax.broadcasted_iota(jnp.int32, (band, width), 0)
        lane = lax.broadcasted_iota(jnp.int32, (band, width), 1)
        zonal, merid = own_ref[:, 0:1], own_ref[:, 1:2]
        east = jnp.where(lane < width - 1, zonal, 0.0)
        west = jnp.where(lane > 0, zonal, 0.0)
        north = jnp.where(row < band - 1, merid, 0.0)
        south = jnp.where(row > 0, merid, 0.0)
    else:
        (inv_ref,) = refs
    levels = sound_ref.shape[0]
    prev = jnp.zeros(sound_ref.shape[1:], F32)
    for k in range(levels):
        alpha = level_ref[k]
        below = alpha * sound_ref[k]
        above = alpha * sound_ref[k + 1] if k + 1 < levels else jnp.zeros_like(below)
        inv = 1.0 / (1.0 + below + above + below * prev)
        prev = -above * inv
        inv_ref[k] = inv
        if len(refs) > 1:
            u, v = u_ref[k], v_ref[k]
            div = east * pltpu.roll(u, width - 1, 1) - west * pltpu.roll(u, 1, 1)
            base_ref[k] = div + north * pltpu.roll(v, band - 1, 0) - south * pltpu.roll(v, 1, 0)


def factor(level_coef, sound, *winds):
    shape = jax.ShapeDtypeStruct(sound.shape, F32)
    count = 1 + len(winds)
    return pl.pallas_call(
        factor_kernel,
        in_specs=[pl.BlockSpec(memory_space=pltpu.SMEM)] + [pl.BlockSpec(memory_space=pltpu.VMEM)] * count,
        out_shape=[shape] * (2 if winds else 1),
        compiler_params=KERNEL,
        cost_estimate=pl.CostEstimate(flops=10 * sound.size, bytes_accessed=16 * sound.size, transcendentals=0),
        name="factor_columns",
    )(level_coef, sound, *winds)


def border_weights(own_ref, near, nz, shape, first_step):
    band = shape[0]
    me = lax.axis_index("lat")
    low, high = me == nz // 2 - 1, me == nz // 2
    row = lax.broadcasted_iota(jnp.int32, shape, 0)
    merid = jnp.broadcast_to(own_ref[:, 1:2], shape)
    last, first = merid[band - 1:], merid[:1]
    on_v = jnp.where(low & (row == band - 1), merid, jnp.where(high & (row == 0), -merid, 0.0))
    if not first_step:
        v_first = jnp.where(low & (row == band - 1), merid, 0.0)
        v_second = jnp.where(high & (row == 0), -merid, 0.0)
        return v_first, v_second
    inner = jnp.where(low & (row == band - 2), -merid * last, 0.0)
    outer = jnp.where(low & (row == band - 1), -merid * near, 0.0)
    on_first = jnp.where(high & (row == 0), -merid * near, inner)
    on_second = jnp.where(high & (row == 1), -merid * first, outer)
    on_own = -jnp.where(high & (row == 0), -merid * near, outer)
    return on_first, on_second, on_own, on_v


def sweep(level_ref, sound_ref, inv_ref, w_ref, star, w_out, p_out, finish):
    levels = sound_ref.shape[0]
    here = star(0)
    value = None
    for k in range(levels):
        alpha = level_ref[k]
        p_out[k] = here
        if k + 1 < levels:
            upper = star(k + 1)
            rhs = w_ref[k] - alpha * (upper - here)
            here = upper
        else:
            rhs = w_ref[k] + alpha * here
        inv = inv_ref[k]
        scaled = rhs * inv
        value = scaled if value is None else scaled + (alpha * sound_ref[k] * inv) * value
        w_out[k] = value
    upper = w_out[levels - 1]
    for k in range(levels - 1, -1, -1):
        lower = None
        if k:
            lower = w_out[k - 1] + (level_ref[k - 1] * sound_ref[k] * inv_ref[k - 1]) * upper
            w_out[k - 1] = lower
        fresh = p_out[k] - sound_ref[k] * (upper if lower is None else upper - lower)
        p_out[k] = fresh
        finish(k, fresh)
        upper = lower


def column_first_kernel(nz, level_ref, own_ref, sound_ref, inv_ref, base_ref, div_ref, p_ref, w_ref, *refs):
    _, band, width = sound_ref.shape
    per = width // LANES
    if nz:
        edge_ref, w_out, p_out, sum_out, rows_out = refs
        weights = border_weights(own_ref, edge_ref[0, 3:4], nz, (band, width), True)
        odd = lax.axis_index("lat") % 2 == 1
    else:
        w_out, p_out = refs

    def star(k):
        div = base_ref[k] + div_ref[k]
        if nz:
            div += weights[0] * edge_ref[k, 0:1] + weights[1] * edge_ref[k, 1:2]
            div += weights[2] * p_ref[k] + weights[3] * edge_ref[k, 2:3]
        return p_ref[k] - sound_ref[k] * div

    def finish(k, fresh):
        if nz:
            total = p_ref[k] + fresh
            rows_out[k] = jnp.where(odd, total[band - 2:], total[:2])
            for h in range(per):
                sum_out[k, h * band:(h + 1) * band] = total[:, h * LANES:(h + 1) * LANES]

    sweep(level_ref, sound_ref, inv_ref, w_ref, star, w_out, p_out, finish)


def column_last_kernel(nz, level_ref, own_ref, sound_ref, inv_ref, field_ref, p_ref, w_ref, u_ref, v_ref, *refs):
    _, band, width = sound_ref.shape
    per = width // LANES
    zonal = jnp.broadcast_to(own_ref[:, 0:1], (band, width))
    merid = jnp.broadcast_to(own_ref[:, 1:2], (band, width))
    if nz:
        edge_ref, facing_ref, rows_ref, u_out, v_out, w_out, p_out = refs
        near = edge_ref[0, 3:4]
        weights = border_weights(own_ref, near, nz, (band, width), False)
        odd = lax.axis_index("lat") % 2 == 1
        row = lax.broadcasted_iota(jnp.int32, (band, width), 0)
        lane = lax.broadcasted_iota(jnp.int32, (band, width), 1)
    else:
        base_ref, u_out, v_out, w_out, p_out = refs

    def wide(k, at):
        return jnp.concatenate([field_ref[k, at + h * band:at + (h + 1) * band] for h in range(per)], axis=1)

    def star(k):
        if not nz:
            u_out[k] = u_ref[k] - zonal * field_ref[k, band:2 * band]
            v_out[k] = v_ref[k] - merid * field_ref[k, 2 * band:]
            return p_ref[k] - sound_ref[k] * (base_ref[k] + field_ref[k, :band])
        u = u_ref[k] - zonal * wide(k, 0)
        v = v_ref[k] - merid * wide(k, per * band)
        far, mine = facing_ref[k], rows_ref[k]
        v -= weights[0] * far[0:1] + weights[1] * far[1:2]
        u_out[k], v_out[k] = u, v
        at = 2 * per * band
        sides = jnp.concatenate([unfold(field_ref[k, at + 4:at + 8])] * per, axis=1)
        pair = jnp.concatenate([field_ref[k, at + h:at + h + 1] for h in range(per)], axis=1)
        half = edge_ref[k, 2:3] - near * jnp.where(odd, far[1:2] - mine[1:2], mine[0:1] - far[0:1])
        north, south = jnp.where(odd, half, pair), jnp.where(odd, pair, half)
        east = jnp.where(lane == width - 1, sides, pltpu.roll(u, width - 1, 1))
        west = jnp.where(lane == 0, sides, pltpu.roll(u, 1, 1))
        up = jnp.where(row == band - 1, north, pltpu.roll(v, band - 1, 0))
        down = jnp.where(row == 0, south, pltpu.roll(v, 1, 0))
        return p_ref[k] - sound_ref[k] * (zonal * (east - west) + merid * (up - down))

    sweep(level_ref, sound_ref, inv_ref, w_ref, star, w_out, p_out, lambda k, fresh: None)


def column(first, nz, level_coef, own, sound, *operands):
    levels, band, width = sound.shape
    shapes = [jax.ShapeDtypeStruct(sound.shape, F32)] * (2 if first else 4)
    if first and nz:
        shapes.append(jax.ShapeDtypeStruct((levels, width // LANES * band, LANES), F32))
        shapes.append(jax.ShapeDtypeStruct((levels, 2, width), F32))
    return pl.pallas_call(
        functools.partial(column_first_kernel if first else column_last_kernel, nz),
        in_specs=[pl.BlockSpec(memory_space=pltpu.SMEM)] + [pl.BlockSpec(memory_space=pltpu.VMEM)] * (2 + len(operands)),
        out_shape=shapes,
        compiler_params=KERNEL,
        cost_estimate=pl.CostEstimate(flops=20 * sound.size, bytes_accessed=40 * sound.size, transcendentals=0),
        name="column_first" if first else "column_last",
    )(level_coef, own, sound, *operands)


def shifted(block, axis, step):
    count = lax.axis_size(axis)
    return lax.ppermute(block, axis, [(i, (i + step) % count) for i in range(count)])


def exchange(block, halves):
    axes, members = "lon", None
    if halves:
        axes = ("lat", "lon")
        count = lax.axis_size(axes)
        members = np.arange(count).reshape(2, count // 2).tolist()
    return lax.all_to_all(block, axes, split_axis=0, concat_axis=0, axis_index_groups=members, tiled=True)


def swapped(block, first):
    count = lax.axis_size("lat")
    pairs = [(i, i + 1) for i in range(first, count - 1, 2)]
    return lax.ppermute(block, "lat", pairs + [(b, a) for a, b in pairs])


def lat_edges(last, first):
    count = lax.axis_size("lat")
    low = lax.ppermute(last, "lat", [(i, i + 1) for i in range(count - 1)])
    high = lax.ppermute(first, "lat", [(i + 1, i) for i in range(count - 1)])
    return low, high


def program(
    zonal_wind,
    merid_wind,
    vertical_wind,
    pressure,
    zonal_coef,
    merid_coef,
    level_coef,
    sound_coef,
    cutoff,
    filter_mask,
):
    levels, band, width = pressure.shape
    nz, nl = lax.axis_size("lat"), lax.axis_size("lon")
    length = width * nl
    lats = band * nz
    me = lax.axis_index("lat")
    weights, table = tables(length)
    own = jnp.stack([zonal_coef, merid_coef], axis=1)
    limit = jnp.where(filter_mask > 0, cutoff, length).astype(F32)
    per = width // LANES

    if nz == 4 and band == 8 and per <= 4 and levels % (2 * nl) == 0:
        depth = levels // (2 * nl)
        offsets = tuple(z * nl * depth + c for c in range(depth) for z in range(2))
        plan = Plan(True, offsets, depth, nl, per, band, 0, band)
        sent, rows = pack(zonal_coef, merid_coef, pressure, zonal_wind, merid_wind)
        circles = exchange(sent, True)
        edges = swapped(rows, 1)
        limits = lax.dynamic_slice_in_dim(limit, me // 2 * 2 * band, 2 * band)
        limits = jnp.tile(limits, depth)[:, None]
        inv, base = factor(level_coef, sound_coef, zonal_wind, merid_wind, own)
        div = transform(plan, False, limits, weights, table, circles)
        div = exchange(div, True)
        w, p, total, rows = column(True, nz, level_coef, own, sound_coef, inv, base, div, pressure, vertical_wind, edges)
        facing = swapped(rows, 1)
        fields = transform(plan, True, limits, weights, table, exchange(total, True), circles)
        fields = exchange(fields, True)
        return column(False, nz, level_coef, own, sound_coef, inv, fields, p, w, zonal_wind, merid_wind, edges, facing, rows)

    depth, halo = levels // nl, 2
    tall = -(-(band + 2 * halo) // 8) * 8
    plan = Plan(False, tuple(range(depth)), depth, nl, per, tall, halo, band)

    def spread(field):
        low, high = lat_edges(field[:, -halo:], field[:, :halo])
        field = jnp.concatenate([low, field, high], axis=1)
        field = jnp.pad(field, ((0, 0), (0, tall - band - 2 * halo), (0, 0)))
        field = field.reshape(levels, tall, per, LANES).swapaxes(1, 2)
        return exchange(field.reshape(levels, per * tall, LANES), False)

    circles = spread(pressure)
    low, high = lat_edges(own[-halo:], own[:halo])
    v_low, v_high = lat_edges(merid_wind[:, -1:], merid_wind[:, :1])
    row = jnp.arange(lats + 2 * halo) - halo
    limit = jnp.pad(limit, (halo, halo), constant_values=1.0)
    known = jnp.stack([limit, (row < lats - 1).astype(F32), (row > 0).astype(F32)], axis=1)
    known = lax.dynamic_slice_in_dim(known, me * band, band + 2 * halo, 0)
    coefs = jnp.concatenate([known, jnp.concatenate([low, own, high])], axis=1)
    coefs = jnp.tile(jnp.pad(coefs, ((0, tall - band - 2 * halo), (0, 0))), (depth, 1))

    u_low = shifted(zonal_wind[:, :, -1:], "lon", 1)
    u_high = shifted(zonal_wind[:, :, :1], "lon", -1)
    u_diff = jnp.concatenate([zonal_wind[:, :, 1:], u_high], 2) - jnp.concatenate([u_low, zonal_wind[:, :, :-1]], 2)
    v_diff = jnp.concatenate([merid_wind[:, 1:], v_high], 1) - jnp.concatenate([v_low, merid_wind[:, :-1]], 1)
    base = zonal_coef[None, :, None] * u_diff + merid_coef[None, :, None] * v_diff

    (inv,) = factor(level_coef, sound_coef)
    div = transform(plan, False, coefs, weights, table, circles)
    div = exchange(div, False)
    w, p = column(True, 0, level_coef, own, sound_coef, inv, base, div, pressure, vertical_wind)
    fields = transform(plan, True, coefs, weights, table, spread(pressure + p))
    fields = exchange(fields, False)
    return column(False, 0, level_coef, own, sound_coef, inv, fields, p, w, zonal_wind, merid_wind, base)


def solution(mesh):
    spec = P(None, "lat", "lon")
    in_specs = (spec, spec, spec, spec, P("lat"), P("lat"), P(), spec, P(), P())
    return jax.shard_map(program, mesh=mesh, in_specs=in_specs, out_specs=(spec,) * 4, check_vma=False)
```

```python
import functools
import math
from typing import NamedTuple

import jax
import jax.numpy as jnp
import numpy as np
from jax import lax
from jax.experimental import pallas as pl
from jax.experimental.pallas import tpu as pltpu
from jax.sharding import PartitionSpec as P


LANES = 128
F32 = jnp.float32
BF16 = jnp.bfloat16
KERNEL = pltpu.CompilerParams(vmem_limit_bytes=8 << 20)
ALONE = pltpu.CompilerParams(vmem_limit_bytes=60 << 20)


class Plan(NamedTuple):
    packed: bool
    bands: int
    nl: int
    depth: int
    per: int
    tall: int
    skip: int
    band: int

    def fields(self, full):
        if not full:
            return "d"
        return "uv" if self.packed else "duv"


def cmul_const(re, im, cr, ci):
    if im is None:
        return (re * cr if cr != 0.0 else None, re * ci if ci != 0.0 else None)
    return (re * cr - im * ci, re * ci + im * cr)


def add(a, b):
    if a is None:
        return b
    return a if b is None else a + b


def sub(a, b):
    if b is None:
        return a
    return -b if a is None else a - b


def neg(a):
    return None if a is None else -a


def unit(num, den):
    turn = num % den
    table = {0: (1.0, 0.0), den / 4: (0.0, 1.0), den / 2: (-1.0, 0.0), 3 * den / 4: (0.0, -1.0)}
    if turn in table:
        return table[turn]
    angle = 2.0 * math.pi * turn / den
    return math.cos(angle), math.sin(angle)


def rotate(z, num, den):
    cr, ci = unit(num, den)
    re, im = z
    if (cr, ci) == (1.0, 0.0):
        return z
    if (cr, ci) == (0.0, 1.0):
        return (neg(im), re)
    if (cr, ci) == (0.0, -1.0):
        return (im, neg(re))
    return cmul_const(re, im, cr, ci)


def real_dft(pieces):
    n = len(pieces)
    if n == 1:
        return [(pieces[0], None)]
    even, odd = real_dft(pieces[0::2]), real_dft(pieces[1::2])
    out = [None] * (n // 2 + 1)
    for s in range(n // 4 + 1 if n > 2 else 1):
        er, ei = even[s]
        tr, ti = rotate(odd[s], -s, n)
        out[n // 2 - s] = (sub(er, tr), sub(ti, ei))
        out[s] = (add(er, tr), add(ei, ti))
    return out


def real_dft_inverse(groups):
    n = 2 * (len(groups) - 1)
    if n == 0:
        return [groups[0][0]]
    if n == 2:
        a, b = groups[0][0], groups[1][0]
        return [a + b, a - b]
    even, odd = [], []
    for s in range(n // 4 + 1):
        ar, ai = groups[s]
        br, bi = groups[n // 2 - s]
        even.append((add(ar, br), sub(ai, bi)))
        odd.append(rotate((sub(ar, br), add(ai, bi)), s, n))
    even[0] = (even[0][0], None)
    odd[0] = (odd[0][0], None)
    even[-1] = (even[-1][0], None)
    odd[-1] = (odd[-1][0], None)
    out = [None] * n
    out[0::2] = real_dft_inverse(even)
    out[1::2] = real_dft_inverse(odd)
    return out


def tables(length):
    pieces = length // LANES
    groups = pieces // 2 + 1
    lane = np.arange(LANES)
    angle = 2.0 * np.pi / LANES * (np.outer(lane, lane) % LANES)
    cos, sin = np.cos(angle), np.sin(angle)
    matrix = np.block([[cos, -sin], [sin, cos]])

    def halves(m):
        m = m.astype(np.float32)
        high = m.astype(BF16)
        return np.stack([high, (m - high.astype(np.float32)).astype(BF16)])

    weights = np.stack([halves(matrix), halves(matrix.T)])
    s = np.arange(groups)[:, None]
    turn = 2.0 * np.pi / length * (s * lane[None, :])
    wavenum = pieces * lane[None, :] + s
    wavenum = np.minimum(wavenum, length - wavenum).astype(np.float64)
    slope = 2.0 * np.sin(2.0 * np.pi / length * (pieces * lane[None, :] + s))
    rows = np.stack([np.cos(turn), np.sin(turn), wavenum, 1.0 / np.maximum(wavenum, 1.0) ** 2, slope])
    return weights, rows.astype(np.float32)


def transform_kernel(plan, full, x_ref, *refs):
    extra_ref = x_ref
    if plan.packed and full:
        extra_ref, refs = refs[0], refs[1:]
    coef_ref, weight_ref, table_ref, result_ref, lhs_ref, spec_ref, work_ref, out_ref, sems = refs
    bands, nl, depth, per = plan.bands, plan.nl, plan.depth, plan.per
    tall, skip, band = plan.tall, plan.skip, plan.band
    stacks = depth * bands
    pieces = nl * per
    groups = pieces // 2 + 1
    rows = stacks * tall
    length = pieces * LANES
    spot = depth * per * tall

    def tile(c, z, l, h):
        at = (c * per + h) * tall
        return x_ref[z * nl + l, at:at + tall]

    def edge_tile(c, z, l):
        return unfold(extra_ref[z * nl + l % nl, spot + 4:spot + 8], c)

    def product(which, start):
        high, low = (lhs_ref[i, start:start + groups * rows] for i in range(2))
        total = jnp.dot(high, weight_ref[which, 0], preferred_element_type=F32)
        total += jnp.dot(low, weight_ref[which, 0], preferred_element_type=F32)
        return total + jnp.dot(high, weight_ref[which, 1], preferred_element_type=F32)

    def put(row, re, im):
        for half, part in enumerate((re, im)):
            high = part.astype(BF16)
            low = (part - high.astype(F32)).astype(BF16)
            lhs_ref[0, row:row + rows, half * LANES:(half + 1) * LANES] = high
            lhs_ref[1, row:row + rows, half * LANES:(half + 1) * LANES] = low

    chunks = []
    for l in range(nl):
        for h in range(per):
            chunks.append(jnp.concatenate([tile(c, z, l, h) for c in range(depth) for z in range(bands)], axis=0))
    zero = jnp.zeros((rows, LANES), F32)
    for s, (re, im) in enumerate(real_dft(chunks)):
        if s:
            cr, ci = table_ref[0, s:s + 1], table_ref[1, s:s + 1]
            if im is None:
                re, im = re * cr, -re * ci
            else:
                re, im = re * cr + im * ci, im * cr - re * ci
        put(s * rows, re, zero if im is None else im)
    spec_ref[...] = product(0, 0)

    def column(a):
        return jnp.broadcast_to(a, (a.shape[0], LANES))

    if plan.packed:
        limit = column(coef_ref[...])
        place = lax.broadcasted_iota(jnp.int32, (rows, LANES), 0) % (bands * tall)
        has_up = jnp.where(place < bands * tall - 1, 1.0, 0.0)
        has_down = jnp.where(place > 0, 1.0, 0.0)
        pair = [edge_tile(0, z, 0) for z in range(bands)]
        zonal = jnp.concatenate([column(t[:, 1:2]) for t in pair] * depth, axis=0)
        merid = jnp.concatenate([column(t[:, 2:3]) for t in pair] * depth, axis=0)
    else:
        limit, has_up, has_down, zonal, merid = (column(coef_ref[:, i:i + 1]) for i in range(5))
    zonal2, merid_up, merid_down = zonal * zonal, merid * has_up, merid * has_down
    limit2 = limit * limit

    def above(a):
        return pltpu.roll(a, rows - 1, 0)

    def below(a):
        return pltpu.roll(a, 1, 0)

    for s in range(groups):
        wavenum, inverse2, slope = (table_ref[i, s:s + 1] for i in (2, 3, 4))
        factor = jnp.where(wavenum > limit, limit2 * inverse2, 1.0)
        parts = [spec_ref[s * rows:(s + 1) * rows, half * LANES:(half + 1) * LANES] for half in (0, 1)]
        spread2 = zonal2 * (slope * slope)
        filtered = [factor * part for part in parts]
        merids, divs = [], []
        for part, filt in zip(parts, filtered):
            across = factor * (has_up * above(part) - has_down * below(part))
            flux = merid * across
            merids.append(across)
            divs.append(spread2 * filt - merid_up * above(flux) + merid_down * below(flux))
        spectra = {"d": divs, "u": (-slope * filtered[1], slope * filtered[0]), "v": merids}
        for field, name in enumerate(plan.fields(full)):
            put((field * groups + s) * rows, *spectra[name])

    row = lax.broadcasted_iota(jnp.int32, (band, LANES), 0)
    lane = lax.broadcasted_iota(jnp.int32, (band, LANES), 1)
    cells = [(c, z, l) for c in range(depth) for z in range(bands) for l in range(nl)]

    def latitudes(c, z):
        first = (c * bands + z) * tall + skip
        return slice(first, first + band)

    leaving = []

    def leave(start, size):
        part = (slice(None), pl.ds(start, size))
        move = pltpu.make_async_copy(out_ref.at[part], result_ref.at[part], sems.at[len(leaving)])
        move.start()
        leaving.append(move)

    results = []
    for field in range(len(plan.fields(full))):
        base = field * groups * rows
        work_ref[...] = product(1, base)
        spectrum = []
        for s in range(groups):
            re = work_ref[s * rows:(s + 1) * rows, :LANES]
            im = work_ref[s * rows:(s + 1) * rows, LANES:]
            if s:
                cr, ci = table_ref[0, s:s + 1], table_ref[1, s:s + 1]
                re, im = re * cr - im * ci, (None if s == groups - 1 else re * ci + im * cr)
            else:
                im = None
            spectrum.append((re, im))
        result = [piece * (1.0 / length) for piece in real_dft_inverse(spectrum)]
        results.append(result)
        for c, z, l in cells:
            own = latitudes(c, z)
            if plan.packed and not full:
                side = band - 1 if z % 2 == 0 else 0
                v_weight = jnp.where(row == side, merid[own] if z % 2 == 0 else -merid[own], 0.0)
                at = spot + c * per
            for h in range(per):
                value = result[l * per + h][own]
                if plan.packed and full:
                    start = ((field * depth + c) * per + h) * band
                    out_ref[z * nl + l, start:start + band] = value
                    continue
                if plan.packed:
                    value += v_weight * extra_ref[(z ^ 1) * nl + l, at + h:at + h + 1]
                    if h == 0:
                        value += jnp.where(lane == 0, -zonal[own], 0.0) * edge_tile(c, z, l - 1)
                    if h == per - 1:
                        value += jnp.where(lane == LANES - 1, zonal[own], 0.0) * edge_tile(c, z, l + 1)
                start = (c * len(plan.fields(full)) + field) * band
                out_ref[z * nl + l, start:start + band, h * LANES:(h + 1) * LANES] = value
        if plan.packed and full:
            leave(field * depth * per * band, depth * per * band)
    if plan.packed and full:
        u, v = results
        base = 2 * depth * per * band
        for z in range(bands):
            for l in range(nl):
                edge = None
                for c in range(depth):
                    own = latitudes(c, z)
                    before = u[(l * per - 1) % pieces][own]
                    after = u[(l * per + per) % pieces][own]
                    before = edge_tile(c, z, l - 1) - zonal[own] * pltpu.roll(before, 1, 1)
                    after = edge_tile(c, z, l + 1) - zonal[own] * pltpu.roll(after, LANES - 1, 1)
                    sides = jnp.where(lane == 0, before, jnp.where(lane == LANES - 1, after, 0.0))
                    edge = sides if c == 0 else edge + pltpu.roll(sides, c * (LANES // 4), 1)
                    other = latitudes(c, z ^ 1)
                    other = other.start if z % 2 == 0 else other.stop - 1
                    at = c * per
                    for h in range(per):
                        moved = merid[other:other + 1] * v[l * per + h][other:other + 1]
                        known = extra_ref[(z ^ 1) * nl + l, spot + at + h:spot + at + h + 1]
                        out_ref[z * nl + l, base + at + h:base + at + h + 1] = known - moved
                out_ref[z * nl + l, base + 4:base + 8] = fold(edge, row)
                if depth * per < 4:
                    out_ref[z * nl + l, base + depth * per:base + 4] = jnp.zeros((4 - depth * per, LANES), F32)
        leave(base, 8)
    else:
        leave(0, out_ref.shape[1])
    for move in leaving:
        move.wait()


def fold(edge, row):
    edge = jnp.where(row < 4, edge, pltpu.roll(edge, LANES // 2, 1))
    return edge[:4] + edge[4:]


def unfold(part, c):
    tile = jnp.concatenate([part, pltpu.roll(part, LANES // 2, 1)], axis=0)
    return pltpu.roll(tile, LANES - c * (LANES // 4), 1) if c else tile


def transform(plan, full, coefs, weights, table, *operands):
    rows = plan.depth * plan.bands * plan.tall
    fields = len(plan.fields(full))
    groups = table.shape[1]
    count = fields * groups * rows
    blocks, width = operands[0].shape[0], plan.per * LANES
    shape = (blocks, plan.depth * fields * plan.band, width)
    if plan.packed and full:
        shape = (blocks, (2 * plan.depth * plan.per + 1) * plan.band, LANES)
    return pl.pallas_call(
        functools.partial(transform_kernel, plan, full),
        out_specs=pl.BlockSpec(memory_space=pltpu.HBM),
        out_shape=jax.ShapeDtypeStruct(shape, F32),
        scratch_shapes=[
            pltpu.VMEM((2, count, 2 * LANES), BF16),
            pltpu.VMEM((groups * rows, 2 * LANES), F32),
            pltpu.VMEM((groups * rows, 2 * LANES), F32),
            pltpu.VMEM(shape, F32),
            pltpu.SemaphoreType.DMA((3,)),
        ],
        compiler_params=KERNEL,
        cost_estimate=pl.CostEstimate(flops=6 * 2 * 65536 * count, bytes_accessed=32 * blocks * plan.depth * plan.band * width, transcendentals=0),
        name="transform_all" if full else "transform_div",
    )(*operands, coefs, weights, table)


def pack_kernel(zonal_ref, merid_ref, p_ref, u_ref, v_ref, result_ref, far_ref, zonal_s, merid_s, out_ref, rows_ref, u_buf, v_buf, in_sems, out_sems):
    blocks, depth, band, width = p_ref.shape
    per = width // LANES
    parts = in_sems.shape[0] - 1
    size = blocks // parts
    spot = depth * per * band

    def chunk(n):
        at = pl.ds(n * size, size)
        moves = [pltpu.make_async_copy(u_ref.at[at], u_buf.at[at], in_sems.at[n, 0]), pltpu.make_async_copy(v_ref.at[at], v_buf.at[at], in_sems.at[n, 1])]
        for c in range(depth):
            for h in range(per):
                source = p_ref.at[at, c, :, pl.ds(h * LANES, LANES)]
                target = out_ref.at[at, pl.ds((c * per + h) * band, band)]
                moves.append(pltpu.make_async_copy(source, target, in_sems.at[n, len(moves)]))
        return moves

    small = [pltpu.make_async_copy(zonal_ref, zonal_s, in_sems.at[parts, 0]), pltpu.make_async_copy(merid_ref, merid_s, in_sems.at[parts, 1])]
    entering = [chunk(n) for n in range(parts)]
    for move in small + sum(entering, []):
        move.start()
    odd = lax.axis_index("lat") % 2 == 1
    row = lax.broadcasted_iota(jnp.int32, (band, LANES), 0)
    lane = lax.broadcasted_iota(jnp.int32, (band, LANES), 1)
    for move in small:
        move.wait()
    coefs = jnp.zeros((band, LANES), F32)
    for j in range(band):
        coefs = jnp.where(row == j, jnp.where(lane == 1, zonal_s[j], jnp.where(lane == 2, merid_s[j], 0.0)), coefs)
    facing = jnp.full((1, width), jnp.where(odd, merid_s[band - 1], merid_s[0]), F32)
    leaving = []
    for n in range(parts):
        for move in entering[n]:
            move.wait()
        for b in range(n * size, (n + 1) * size):
            edge = coefs
            for c in range(depth):
                west = pltpu.roll(u_buf[b, c, :, width - LANES:], 1, 1)
                east = pltpu.roll(u_buf[b, c, :, :LANES], LANES - 1, 1)
                sides = jnp.where(lane == 0, west, jnp.where(lane == LANES - 1, east, 0.0))
                edge = edge + (pltpu.roll(sides, c * (LANES // 4), 1) if c else sides)
                k = b * depth + c
                for h in range(per):
                    lanes = slice(h * LANES, (h + 1) * LANES)
                    at = (c * per + h) * band
                    top, bottom = v_buf[b, c, :1, lanes], v_buf[b, c, band - 1:, lanes]
                    out_ref[b, spot + c * per + h:spot + c * per + h + 1] = jnp.where(odd, top, bottom)
                    rows_ref[k, 2:3, lanes] = jnp.where(odd, bottom, top)
                    rows_ref[k, :2, lanes] = jnp.where(odd, out_ref[b, at + band - 2:at + band], out_ref[b, at:at + 2])
                rows_ref[k, 3:4] = facing
            out_ref[b, spot + 4:spot + 8] = fold(edge, row)
            if depth * per < 4:
                out_ref[b, spot + depth * per:spot + 4] = jnp.zeros((4 - depth * per, LANES), F32)
        at = pl.ds(n * size, size)
        leaving.append(pltpu.make_async_copy(out_ref.at[at], result_ref.at[at], out_sems.at[n]))
        leaving[-1].start()
    leaving.append(pltpu.make_async_copy(rows_ref, far_ref, out_sems.at[parts]))
    leaving[-1].start()
    for move in leaving:
        move.wait()


def pack(zonal, merid, p, u, v):
    blocks, depth, band, width = p.shape
    per = width // LANES
    shape = (blocks, (depth * per + 1) * band, LANES)
    rows = (blocks * depth, 4, width)
    parts = 4 if blocks % 4 == 0 else 1
    hbm = pl.BlockSpec(memory_space=pltpu.HBM)
    return pl.pallas_call(
        pack_kernel,
        in_specs=[hbm] * 5,
        out_specs=[hbm, hbm],
        out_shape=[jax.ShapeDtypeStruct(shape, F32), jax.ShapeDtypeStruct(rows, F32)],
        scratch_shapes=[
            pltpu.SMEM((band,), F32),
            pltpu.SMEM((band,), F32),
            pltpu.VMEM(shape, F32),
            pltpu.VMEM(rows, F32),
            pltpu.VMEM(p.shape, F32),
            pltpu.VMEM(p.shape, F32),
            pltpu.SemaphoreType.DMA((parts + 1, 2 + depth * per)),
            pltpu.SemaphoreType.DMA((parts + 1,)),
        ],
        compiler_params=ALONE,
        cost_estimate=pl.CostEstimate(flops=p.size, bytes_accessed=16 * p.size, transcendentals=0),
        name="pack_circles",
    )(zonal, merid, p, u, v)


def factor_kernel(level_ref, sound_ref, *refs):
    if len(refs) > 1:
        u_ref, v_ref, own_ref, inv_ref, base_ref = refs
        band, width = u_ref.shape[1:]
        row = lax.broadcasted_iota(jnp.int32, (band, width), 0)
        lane = lax.broadcasted_iota(jnp.int32, (band, width), 1)
        zonal, merid = own_ref[:, 0:1], own_ref[:, 1:2]
        east = jnp.where(lane < width - 1, zonal, 0.0)
        west = jnp.where(lane > 0, zonal, 0.0)
        north = jnp.where(row < band - 1, merid, 0.0)
        south = jnp.where(row > 0, merid, 0.0)
    else:
        (inv_ref,) = refs
    levels = sound_ref.shape[0]
    prev = jnp.zeros(sound_ref.shape[1:], F32)
    for k in range(levels):
        alpha = level_ref[k:k + 1]
        below = alpha * sound_ref[k]
        above = alpha * sound_ref[k + 1] if k + 1 < levels else jnp.zeros_like(below)
        inv = 1.0 / (1.0 + below + above + below * prev)
        prev = -above * inv
        inv_ref[k] = inv
        if len(refs) > 1:
            u, v = u_ref[k], v_ref[k]
            div = east * pltpu.roll(u, width - 1, 1) - west * pltpu.roll(u, 1, 1)
            base_ref[k] = div + north * pltpu.roll(v, band - 1, 0) - south * pltpu.roll(v, 1, 0)


def factor(level_coef, sound, *winds):
    shape = jax.ShapeDtypeStruct(sound.shape, F32)
    count = 1 + len(winds)
    return pl.pallas_call(
        factor_kernel,
        in_specs=[pl.BlockSpec(memory_space=pltpu.VMEM)] * (1 + count),
        out_shape=[shape] * (2 if winds else 1),
        compiler_params=KERNEL,
        cost_estimate=pl.CostEstimate(flops=10 * sound.size, bytes_accessed=16 * sound.size, transcendentals=0),
        name="factor_columns",
    )(level_coef, sound, *winds)


def border_weights(own_ref, near, nz, shape, first_step):
    band = shape[0]
    me = lax.axis_index("lat")
    low, high = me == nz // 2 - 1, me == nz // 2
    row = lax.broadcasted_iota(jnp.int32, shape, 0)
    merid = jnp.broadcast_to(own_ref[:, 1:2], shape)
    last, first = merid[band - 1:], merid[:1]
    on_v = jnp.where(low & (row == band - 1), merid, jnp.where(high & (row == 0), -merid, 0.0))
    if not first_step:
        v_first = jnp.where(low & (row == band - 1), merid, 0.0)
        v_second = jnp.where(high & (row == 0), -merid, 0.0)
        return v_first, v_second
    inner = jnp.where(low & (row == band - 2), -merid * last, 0.0)
    outer = jnp.where(low & (row == band - 1), -merid * near, 0.0)
    on_first = jnp.where(high & (row == 0), -merid * near, inner)
    on_second = jnp.where(high & (row == 1), -merid * first, outer)
    on_own = -jnp.where(high & (row == 0), -merid * near, outer)
    return on_first, on_second, on_own, on_v


def sweep(level_ref, sound_ref, inv_ref, w_ref, star, w_out, p_out, finish):
    levels = sound_ref.shape[0]
    here = star(0)
    value = None
    for k in range(levels):
        alpha = level_ref[k:k + 1]
        p_out[k] = here
        if k + 1 < levels:
            upper = star(k + 1)
            rhs = w_ref[k] - alpha * (upper - here)
            here = upper
        else:
            rhs = w_ref[k] + alpha * here
        inv = inv_ref[k]
        scaled = rhs * inv
        value = scaled if value is None else scaled + (alpha * sound_ref[k] * inv) * value
        w_out[k] = value
    upper = w_out[levels - 1]
    for k in range(levels - 1, -1, -1):
        lower = None
        if k:
            lower = w_out[k - 1] + (level_ref[k - 1:k] * sound_ref[k] * inv_ref[k - 1]) * upper
            w_out[k - 1] = lower
        fresh = p_out[k] - sound_ref[k] * (upper if lower is None else upper - lower)
        p_out[k] = fresh
        finish(k, fresh)
        upper = lower


def column_first_kernel(nz, level_ref, own_ref, sound_ref, inv_ref, base_ref, div_ref, p_ref, w_ref, *refs):
    levels, band, width = sound_ref.shape
    per = width // LANES
    if nz:
        edge_ref, w_out, p_out, sum_out, rows_out = refs
        depth = levels // sum_out.shape[0]
        weights = border_weights(own_ref, edge_ref[0, 3:4], nz, (band, width), True)
        odd = lax.axis_index("lat") % 2 == 1
    else:
        w_out, p_out = refs

    def star(k):
        div = base_ref[k] + div_ref[k]
        if nz:
            div += weights[0] * edge_ref[k, 0:1] + weights[1] * edge_ref[k, 1:2]
            div += weights[2] * p_ref[k] + weights[3] * edge_ref[k, 2:3]
        return p_ref[k] - sound_ref[k] * div

    def finish(k, fresh):
        if nz:
            total = p_ref[k] + fresh
            rows_out[k] = jnp.where(odd, total[band - 2:], total[:2])
            for h in range(per):
                at = (k % depth * per + h) * band
                sum_out[k // depth, at:at + band] = total[:, h * LANES:(h + 1) * LANES]

    sweep(level_ref, sound_ref, inv_ref, w_ref, star, w_out, p_out, finish)


def column_last_kernel(nz, level_ref, own_ref, sound_ref, inv_ref, field_ref, p_ref, w_ref, u_ref, v_ref, *refs):
    levels, band, width = sound_ref.shape
    per = width // LANES
    zonal = jnp.broadcast_to(own_ref[:, 0:1], (band, width))
    merid = jnp.broadcast_to(own_ref[:, 1:2], (band, width))
    if nz:
        edge_ref, facing_ref, rows_ref, refs = refs[0], refs[1], refs[2], refs[3:]
        depth = levels // field_ref.shape[0]
        near = edge_ref[0, 3:4]
        weights = border_weights(own_ref, near, nz, (band, width), False)
        odd = lax.axis_index("lat") % 2 == 1
        row = lax.broadcasted_iota(jnp.int32, (band, width), 0)
        lane = lax.broadcasted_iota(jnp.int32, (band, width), 1)
    else:
        base_ref, refs = refs[0], refs[1:]
    u_out, v_out, w_out, p_out = refs[4:8]
    sems = refs[8]
    leaving = []
    size = levels // 4

    def leave(out, start):
        part = pl.ds(start, size)
        move = pltpu.make_async_copy(refs[4 + out].at[part], refs[out].at[part], sems.at[len(leaving)])
        move.start()
        leaving.append(move)

    def wide(k, field):
        at = (field * depth + k % depth) * per * band
        return jnp.concatenate([field_ref[k // depth, at + h * band:at + (h + 1) * band] for h in range(per)], axis=1)

    def star(k):
        result = new_star(k)
        if (k + 1) % size == 0:
            leave(0, k + 1 - size)
            leave(1, k + 1 - size)
        return result

    def finish(k, fresh):
        if k % size == 0:
            leave(2, k)
            leave(3, k)

    def new_star(k):
        if not nz:
            u_out[k] = u_ref[k] - zonal * field_ref[k, band:2 * band]
            v_out[k] = v_ref[k] - merid * field_ref[k, 2 * band:]
            return p_ref[k] - sound_ref[k] * (base_ref[k] + field_ref[k, :band])
        u = u_ref[k] - zonal * wide(k, 0)
        v = v_ref[k] - merid * wide(k, 1)
        far, mine = facing_ref[k], rows_ref[k]
        v -= weights[0] * far[0:1] + weights[1] * far[1:2]
        u_out[k], v_out[k] = u, v
        b, c, at = k // depth, k % depth, 2 * depth * per * band
        sides = jnp.concatenate([unfold(field_ref[b, at + 4:at + 8], c)] * per, axis=1)
        at += c * per
        pair = jnp.concatenate([field_ref[b, at + h:at + h + 1] for h in range(per)], axis=1)
        half = edge_ref[k, 2:3] - near * jnp.where(odd, far[1:2] - mine[1:2], mine[0:1] - far[0:1])
        north, south = jnp.where(odd, half, pair), jnp.where(odd, pair, half)
        east = jnp.where(lane == width - 1, sides, pltpu.roll(u, width - 1, 1))
        west = jnp.where(lane == 0, sides, pltpu.roll(u, 1, 1))
        up = jnp.where(row == band - 1, north, pltpu.roll(v, band - 1, 0))
        down = jnp.where(row == 0, south, pltpu.roll(v, 1, 0))
        return p_ref[k] - sound_ref[k] * (zonal * (east - west) + merid * (up - down))

    sweep(level_ref, sound_ref, inv_ref, w_ref, star, w_out, p_out, finish)
    for move in leaving:
        move.wait()


def column(first, nz, depth, level_coef, own, sound, *operands):
    levels, band, width = sound.shape
    shapes = [jax.ShapeDtypeStruct(sound.shape, F32)] * (2 if first else 4)
    if first and nz:
        shapes.append(jax.ShapeDtypeStruct((levels // depth, depth * (width // LANES) * band, LANES), F32))
        shapes.append(jax.ShapeDtypeStruct((levels, 2, width), F32))
    extra = {}
    if not first:
        extra["scratch_shapes"] = [pltpu.VMEM(sound.shape, F32)] * 4 + [pltpu.SemaphoreType.DMA((16,))]
    return pl.pallas_call(
        functools.partial(column_first_kernel if first else column_last_kernel, nz),
        in_specs=[pl.BlockSpec(memory_space=pltpu.VMEM)] * (3 + len(operands)),
        out_specs=[pl.BlockSpec(memory_space=pltpu.VMEM if first else pltpu.HBM)] * len(shapes),
        out_shape=shapes,
        compiler_params=KERNEL,
        cost_estimate=pl.CostEstimate(flops=20 * sound.size, bytes_accessed=40 * sound.size, transcendentals=0),
        name="column_first" if first else "column_last",
        **extra,
    )(level_coef, own, sound, *operands)


def shifted(block, axis, step):
    count = lax.axis_size(axis)
    return lax.ppermute(block, axis, [(i, (i + step) % count) for i in range(count)])


def exchange(block, halves):
    axes, members = "lon", None
    if halves:
        axes = ("lat", "lon")
        count = lax.axis_size(axes)
        members = np.arange(count).reshape(2, count // 2).tolist()
    return lax.all_to_all(block, axes, split_axis=0, concat_axis=0, axis_index_groups=members, tiled=True)


def swapped(block, first):
    count = lax.axis_size("lat")
    pairs = [(i, i + 1) for i in range(first, count - 1, 2)]
    return lax.ppermute(block, "lat", pairs + [(b, a) for a, b in pairs])


def lat_edges(last, first):
    count = lax.axis_size("lat")
    low = lax.ppermute(last, "lat", [(i, i + 1) for i in range(count - 1)])
    high = lax.ppermute(first, "lat", [(i + 1, i) for i in range(count - 1)])
    return low, high


def program(
    zonal_wind,
    merid_wind,
    vertical_wind,
    pressure,
    zonal_coef,
    merid_coef,
    level_coef,
    sound_coef,
    cutoff,
    filter_mask,
):
    levels, band, width = pressure.shape
    nz, nl = lax.axis_size("lat"), lax.axis_size("lon")
    length = width * nl
    lats = band * nz
    me = lax.axis_index("lat")
    weights, table = tables(length)
    level_rows = jnp.broadcast_to(level_coef[:, None], (levels, width))
    own = jnp.stack([zonal_coef, merid_coef], axis=1)
    limit = jnp.where(filter_mask > 0, cutoff, length).astype(F32)
    per = width // LANES

    depth = levels // (2 * nl)
    if nz == 4 and band == 8 and 1 <= depth <= 2 and depth * per <= 4 and levels == 2 * nl * depth:
        plan = Plan(True, 2, nl, depth, per, band, 0, band)
        blocked = [a.reshape(levels // depth, depth, band, width) for a in (pressure, zonal_wind, merid_wind)]
        sent, rows = pack(zonal_coef, merid_coef, *blocked)
        circles = exchange(sent, True)
        edges = swapped(rows, 1)
        limits = lax.dynamic_slice_in_dim(limit, me // 2 * 2 * band, 2 * band)
        limits = jnp.tile(limits, depth)[:, None]
        inv, base = factor(level_rows, sound_coef, zonal_wind, merid_wind, own)
        div = transform(plan, False, limits, weights, table, circles)
        div = exchange(div, True).reshape(levels, band, width)
        w, p, total, rows = column(True, nz, depth, level_rows, own, sound_coef, inv, base, div, pressure, vertical_wind, edges)
        facing = swapped(rows, 1)
        fields = transform(plan, True, limits, weights, table, exchange(total, True), circles)
        fields = exchange(fields, True)
        return column(False, nz, depth, level_rows, own, sound_coef, inv, fields, p, w, zonal_wind, merid_wind, edges, facing, rows)

    depth, halo = levels // nl, 2
    tall = -(-(band + 2 * halo) // 8) * 8
    plan = Plan(False, 1, nl, depth, per, tall, halo, band)

    def spread(field):
        low, high = lat_edges(field[:, -halo:], field[:, :halo])
        field = jnp.concatenate([low, field, high], axis=1)
        field = jnp.pad(field, ((0, 0), (0, tall - band - 2 * halo), (0, 0)))
        field = field.reshape(levels, tall, per, LANES).swapaxes(1, 2)
        return exchange(field.reshape(nl, depth * per * tall, LANES), False)

    circles = spread(pressure)
    low, high = lat_edges(own[-halo:], own[:halo])
    v_low, v_high = lat_edges(merid_wind[:, -1:], merid_wind[:, :1])
    row = jnp.arange(lats + 2 * halo) - halo
    limit = jnp.pad(limit, (halo, halo), constant_values=1.0)
    known = jnp.stack([limit, (row < lats - 1).astype(F32), (row > 0).astype(F32)], axis=1)
    known = lax.dynamic_slice_in_dim(known, me * band, band + 2 * halo, 0)
    coefs = jnp.concatenate([known, jnp.concatenate([low, own, high])], axis=1)
    coefs = jnp.tile(jnp.pad(coefs, ((0, tall - band - 2 * halo), (0, 0))), (depth, 1))

    u_low = shifted(zonal_wind[:, :, -1:], "lon", 1)
    u_high = shifted(zonal_wind[:, :, :1], "lon", -1)
    u_diff = jnp.concatenate([zonal_wind[:, :, 1:], u_high], 2) - jnp.concatenate([u_low, zonal_wind[:, :, :-1]], 2)
    v_diff = jnp.concatenate([merid_wind[:, 1:], v_high], 1) - jnp.concatenate([v_low, merid_wind[:, :-1]], 1)
    base = zonal_coef[None, :, None] * u_diff + merid_coef[None, :, None] * v_diff

    (inv,) = factor(level_rows, sound_coef)
    div = transform(plan, False, coefs, weights, table, circles)
    div = exchange(div, False).reshape(levels, band, width)
    w, p = column(True, 0, depth, level_rows, own, sound_coef, inv, base, div, pressure, vertical_wind)
    fields = transform(plan, True, coefs, weights, table, spread(pressure + p))
    fields = exchange(fields, False).reshape(levels, 3 * band, width)
    return column(False, 0, depth, level_rows, own, sound_coef, inv, fields, p, w, zonal_wind, merid_wind, base)


def solution(mesh):
    spec = P(None, "lat", "lon")
    in_specs = (spec, spec, spec, spec, P("lat"), P("lat"), P(), spec, P(), P())
    return jax.shard_map(program, mesh=mesh, in_specs=in_specs, out_specs=(spec,) * 4, check_vma=False)
```

```python
import functools
import math
from typing import NamedTuple

import jax
import jax.numpy as jnp
import numpy as np
from jax import lax
from jax.experimental import pallas as pl
from jax.experimental.pallas import tpu as pltpu
from jax.sharding import PartitionSpec as P


LANES = 128
F32 = jnp.float32
BF16 = jnp.bfloat16
KERNEL = pltpu.CompilerParams(vmem_limit_bytes=8 << 20)


class Plan(NamedTuple):
    packed: bool
    bands: int
    nl: int
    depth: int
    per: int
    tall: int
    skip: int
    band: int

    def fields(self, full):
        if not full:
            return "d"
        return "uv" if self.packed else "duv"


def cmul_const(re, im, cr, ci):
    if im is None:
        return (re * cr if cr != 0.0 else None, re * ci if ci != 0.0 else None)
    return (re * cr - im * ci, re * ci + im * cr)


def add(a, b):
    if a is None:
        return b
    return a if b is None else a + b


def sub(a, b):
    if b is None:
        return a
    return -b if a is None else a - b


def neg(a):
    return None if a is None else -a


def unit(num, den):
    turn = num % den
    table = {0: (1.0, 0.0), den / 4: (0.0, 1.0), den / 2: (-1.0, 0.0), 3 * den / 4: (0.0, -1.0)}
    if turn in table:
        return table[turn]
    angle = 2.0 * math.pi * turn / den
    return math.cos(angle), math.sin(angle)


def rotate(z, num, den):
    cr, ci = unit(num, den)
    re, im = z
    if (cr, ci) == (1.0, 0.0):
        return z
    if (cr, ci) == (0.0, 1.0):
        return (neg(im), re)
    if (cr, ci) == (0.0, -1.0):
        return (im, neg(re))
    return cmul_const(re, im, cr, ci)


def real_dft(pieces):
    n = len(pieces)
    if n == 1:
        return [(pieces[0], None)]
    even, odd = real_dft(pieces[0::2]), real_dft(pieces[1::2])
    out = [None] * (n // 2 + 1)
    for s in range(n // 4 + 1 if n > 2 else 1):
        er, ei = even[s]
        tr, ti = rotate(odd[s], -s, n)
        out[n // 2 - s] = (sub(er, tr), sub(ti, ei))
        out[s] = (add(er, tr), add(ei, ti))
    return out


def real_dft_inverse(groups):
    n = 2 * (len(groups) - 1)
    if n == 0:
        return [groups[0][0]]
    if n == 2:
        a, b = groups[0][0], groups[1][0]
        return [a + b, a - b]
    even, odd = [], []
    for s in range(n // 4 + 1):
        ar, ai = groups[s]
        br, bi = groups[n // 2 - s]
        even.append((add(ar, br), sub(ai, bi)))
        odd.append(rotate((sub(ar, br), add(ai, bi)), s, n))
    even[0] = (even[0][0], None)
    odd[0] = (odd[0][0], None)
    even[-1] = (even[-1][0], None)
    odd[-1] = (odd[-1][0], None)
    out = [None] * n
    out[0::2] = real_dft_inverse(even)
    out[1::2] = real_dft_inverse(odd)
    return out


def tables(length):
    pieces = length // LANES
    groups = pieces // 2 + 1
    lane = np.arange(LANES)
    angle = 2.0 * np.pi / LANES * (np.outer(lane, lane) % LANES)
    cos, sin = np.cos(angle), np.sin(angle)
    matrix = np.block([[cos, -sin], [sin, cos]])

    def halves(m):
        m = m.astype(np.float32)
        high = m.astype(BF16)
        return np.stack([high, (m - high.astype(np.float32)).astype(BF16)])

    weights = np.stack([halves(matrix), halves(matrix.T)])
    s = np.arange(groups)[:, None]
    turn = 2.0 * np.pi / length * (s * lane[None, :])
    wavenum = pieces * lane[None, :] + s
    wavenum = np.minimum(wavenum, length - wavenum).astype(np.float64)
    slope = 2.0 * np.sin(2.0 * np.pi / length * (pieces * lane[None, :] + s))
    rows = np.stack([np.cos(turn), np.sin(turn), wavenum, 1.0 / np.maximum(wavenum, 1.0) ** 2, slope])
    return weights, rows.astype(np.float32)


def transform_kernel(plan, full, x_ref, *refs):
    if plan.packed:
        own_ref, near_ref, refs = refs[0], refs[1], refs[2:]
    coef_ref, weight_ref, table_ref, result_ref, lhs_ref, spec_ref, work_ref, out_ref, sems = refs
    bands, nl, depth, per = plan.bands, plan.nl, plan.depth, plan.per
    tall, skip, band = plan.tall, plan.skip, plan.band
    stacks = depth * bands
    pieces = nl * per
    groups = pieces // 2 + 1
    rows = stacks * tall
    length = pieces * LANES

    def tile(c, z, l, h):
        return x_ref[z * nl + l, c * tall:(c + 1) * tall, h * LANES:(h + 1) * LANES]

    def product(which, start):
        high, low = (lhs_ref[i, start:start + groups * rows] for i in range(2))
        total = jnp.dot(high, weight_ref[which, 0], preferred_element_type=F32)
        total += jnp.dot(low, weight_ref[which, 0], preferred_element_type=F32)
        return total + jnp.dot(high, weight_ref[which, 1], preferred_element_type=F32)

    def put(row, re, im):
        for half, part in enumerate((re, im)):
            high = part.astype(BF16)
            low = (part - high.astype(F32)).astype(BF16)
            lhs_ref[0, row:row + rows, half * LANES:(half + 1) * LANES] = high
            lhs_ref[1, row:row + rows, half * LANES:(half + 1) * LANES] = low

    chunks = []
    for l in range(nl):
        for h in range(per):
            chunks.append(jnp.concatenate([tile(c, z, l, h) for c in range(depth) for z in range(bands)], axis=0))
    zero = jnp.zeros((rows, LANES), F32)
    for s, (re, im) in enumerate(real_dft(chunks)):
        if s:
            cr, ci = table_ref[0, s:s + 1], table_ref[1, s:s + 1]
            if im is None:
                re, im = re * cr, -re * ci
            else:
                re, im = re * cr + im * ci, im * cr - re * ci
        put(s * rows, re, zero if im is None else im)
    spec_ref[...] = product(0, 0)

    def column(a):
        return jnp.broadcast_to(a, (a.shape[0], LANES))

    if plan.packed:
        limit = coef_ref[...]
        place = lax.broadcasted_iota(jnp.int32, (rows, LANES), 0) % (bands * tall)
        has_up = jnp.where(place < bands * tall - 1, 1.0, 0.0)
        has_down = jnp.where(place > 0, 1.0, 0.0)
        odd = lax.axis_index("lat") % 2 == 1
        own_rows, near_rows = own_ref[...], near_ref[-tall:, :LANES]
        pair = [jnp.where(odd, near_rows, own_rows), jnp.where(odd, own_rows, near_rows)]
        zonal = jnp.concatenate([column(t[:, 0:1]) for t in pair] * depth, axis=0)
        merid = jnp.concatenate([column(t[:, 1:2]) for t in pair] * depth, axis=0)
    else:
        limit, has_up, has_down, zonal, merid = (column(coef_ref[:, i:i + 1]) for i in range(5))
    zonal2, merid_up, merid_down = zonal * zonal, merid * has_up, merid * has_down
    limit2 = limit * limit

    def above(a):
        return pltpu.roll(a, rows - 1, 0)

    def below(a):
        return pltpu.roll(a, 1, 0)

    for s in range(groups):
        wavenum, inverse2, slope = (table_ref[i, s:s + 1] for i in (2, 3, 4))
        factor = jnp.where(wavenum > limit, limit2 * inverse2, 1.0)
        parts = [spec_ref[s * rows:(s + 1) * rows, half * LANES:(half + 1) * LANES] for half in (0, 1)]
        spread2 = zonal2 * (slope * slope)
        filtered = [factor * part for part in parts]
        merids, divs = [], []
        for part, filt in zip(parts, filtered):
            across = factor * (has_up * above(part) - has_down * below(part))
            flux = merid * across
            merids.append(across)
            divs.append(spread2 * filt - merid_up * above(flux) + merid_down * below(flux))
        spectra = {"d": divs, "u": (-slope * filtered[1], slope * filtered[0]), "v": merids}
        for field, name in enumerate(plan.fields(full)):
            put((field * groups + s) * rows, *spectra[name])

    row = lax.broadcasted_iota(jnp.int32, (band, LANES), 0)
    lane = lax.broadcasted_iota(jnp.int32, (band, LANES), 1)
    cells = [(c, z, l) for c in range(depth) for z in range(bands) for l in range(nl)]

    def latitudes(c, z):
        first = (c * bands + z) * tall + skip
        return slice(first, first + band)

    leaving = []

    def leave(start, size):
        part = (slice(None), pl.ds(start, size))
        move = pltpu.make_async_copy(out_ref.at[part], result_ref.at[part], sems.at[len(leaving)])
        move.start()
        leaving.append(move)

    results = []
    for field in range(len(plan.fields(full))):
        base = field * groups * rows
        work_ref[...] = product(1, base)
        spectrum = []
        for s in range(groups):
            re = work_ref[s * rows:(s + 1) * rows, :LANES]
            im = work_ref[s * rows:(s + 1) * rows, LANES:]
            if s:
                cr, ci = table_ref[0, s:s + 1], table_ref[1, s:s + 1]
                re, im = re * cr - im * ci, (None if s == groups - 1 else re * ci + im * cr)
            else:
                im = None
            spectrum.append((re, im))
        result = [piece * (1.0 / length) for piece in real_dft_inverse(spectrum)]
        results.append(result)
        for c, z, l in cells:
            own = latitudes(c, z)
            for h in range(per):
                value = result[l * per + h][own]
                if plan.packed and full:
                    start = ((field * depth + c) * per + h) * band
                    out_ref[z * nl + l, start:start + band] = value
                    continue
                start = (c * len(plan.fields(full)) + field) * band
                out_ref[z * nl + l, start:start + band, h * LANES:(h + 1) * LANES] = value
        if plan.packed and full:
            leave(field * depth * per * band, depth * per * band)
    if plan.packed and full:
        u, v = results
        base = 2 * depth * per * band
        for z in range(bands):
            for l in range(nl):
                edge = None
                for c in range(depth):
                    own = latitudes(c, z)
                    before = u[(l * per - 1) % pieces][own]
                    after = u[(l * per + per) % pieces][own]
                    before = -zonal[own] * pltpu.roll(before, 1, 1)
                    after = -zonal[own] * pltpu.roll(after, LANES - 1, 1)
                    sides = jnp.where(lane == 0, before, jnp.where(lane == LANES - 1, after, 0.0))
                    edge = sides if c == 0 else edge + pltpu.roll(sides, c * (LANES // 4), 1)
                    other = latitudes(c, z ^ 1)
                    other = other.start if z % 2 == 0 else other.stop - 1
                    at = c * per
                    for h in range(per):
                        moved = merid[other:other + 1] * v[l * per + h][other:other + 1]
                        out_ref[z * nl + l, base + at + h:base + at + h + 1] = -moved
                out_ref[z * nl + l, base + 4:base + 8] = fold(edge, row)
                if depth * per < 4:
                    out_ref[z * nl + l, base + depth * per:base + 4] = jnp.zeros((4 - depth * per, LANES), F32)
        leave(base, 8)
    else:
        leave(0, out_ref.shape[1])
    for move in leaving:
        move.wait()


def fold(edge, row):
    edge = jnp.where(row < 4, edge, pltpu.roll(edge, LANES // 2, 1))
    return edge[:4] + edge[4:]


def unfold(part, c):
    tile = jnp.concatenate([part, pltpu.roll(part, LANES // 2, 1)], axis=0)
    return pltpu.roll(tile, LANES - c * (LANES // 4), 1) if c else tile


def transform(plan, full, coefs, weights, table, *operands):
    rows = plan.depth * plan.bands * plan.tall
    fields = len(plan.fields(full))
    groups = table.shape[1]
    count = fields * groups * rows
    blocks, width = operands[0].shape[0], plan.per * LANES
    shape = (blocks, plan.depth * fields * plan.band, width)
    if plan.packed and full:
        shape = (blocks, (2 * plan.depth * plan.per + 1) * plan.band, LANES)
    return pl.pallas_call(
        functools.partial(transform_kernel, plan, full),
        out_specs=pl.BlockSpec(memory_space=pltpu.HBM),
        out_shape=jax.ShapeDtypeStruct(shape, F32),
        scratch_shapes=[
            pltpu.VMEM((2, count, 2 * LANES), BF16),
            pltpu.VMEM((groups * rows, 2 * LANES), F32),
            pltpu.VMEM((groups * rows, 2 * LANES), F32),
            pltpu.VMEM(shape, F32),
            pltpu.SemaphoreType.DMA((3,)),
        ],
        compiler_params=KERNEL,
        cost_estimate=pl.CostEstimate(flops=6 * 2 * 65536 * count, bytes_accessed=32 * blocks * plan.depth * plan.band * width, transcendentals=0),
        name="transform_all" if full else "transform_div",
    )(*operands, coefs, weights, table)


def factor_kernel(level_ref, sound_ref, *refs):
    levels, band, width = sound_ref.shape
    full = len(refs) > 1
    if full:
        u_ref, v_ref, own_ref, inv_ref, base_ref = refs
        row = lax.broadcasted_iota(jnp.int32, (band, width), 0)
        lane = lax.broadcasted_iota(jnp.int32, (band, width), 1)
        zonal, merid = own_ref[:, 0:1], own_ref[:, 1:2]
        east = jnp.where(lane < width - 1, zonal, 0.0)
        west = jnp.where(lane > 0, zonal, 0.0)
        north = jnp.where(row < band - 1, merid, 0.0)
        south = jnp.where(row > 0, merid, 0.0)
    else:
        (inv_ref,) = refs
    prev = jnp.zeros((band, width), F32)
    for k in range(levels):
        alpha = level_ref[k:k + 1]
        below = alpha * sound_ref[k]
        above = alpha * sound_ref[k + 1] if k + 1 < levels else jnp.zeros_like(below)
        inv = 1.0 / (1.0 + below + above + below * prev)
        prev = -above * inv
        inv_ref[k] = inv
        if full:
            u, v = u_ref[k], v_ref[k]
            div = east * pltpu.roll(u, width - 1, 1) - west * pltpu.roll(u, 1, 1)
            base_ref[k] = div + north * pltpu.roll(v, band - 1, 0) - south * pltpu.roll(v, 1, 0)


def edges_kernel(depth, bands, zonal_ref, merid_ref, level_ref, cutoff_ref, mask_ref, p_ref, u_ref, v_ref, *refs):
    pair_ref, half_ref, side_ref, own_ref, rows_ref, limit_ref = refs[:6]
    smalls, (p_buf, u_buf, v_buf), sems = refs[6:11], refs[11:14], refs[14]
    levels, band, width = u_buf.shape
    moves = []
    for source, target in zip((zonal_ref, merid_ref, level_ref, cutoff_ref, mask_ref, p_ref, u_ref, v_ref), (*smalls, p_buf, u_buf, v_buf)):
        moves.append(pltpu.make_async_copy(source, target, sems.at[len(moves)]))
        moves[-1].start()
    for move in moves[:5]:
        move.wait()
    zonal_s, merid_s, level_s, cutoff_s, mask_s = smalls
    me = lax.axis_index("lat")
    odd = me % 2 == 1
    row = lax.broadcasted_iota(jnp.int32, (band, LANES), 0)
    lane = lax.broadcasted_iota(jnp.int32, (band, LANES), 1)
    own = jnp.zeros((band, LANES), F32)
    for j in range(band):
        own = jnp.where(row == j, jnp.where(lane == 0, zonal_s[j], jnp.where(lane == 1, merid_s[j], 0.0)), own)
    own_ref[...] = own
    pair_ref[levels:, :LANES] = own
    if width > LANES:
        pair_ref[levels:, LANES:] = jnp.zeros((band, width - LANES), F32)
    for k in range(levels):
        rows_ref[k:k + 1] = jnp.full((1, width), level_s[k], F32)
    start = me // bands * bands * band
    for z in range(bands):
        limit = jnp.zeros((band, LANES), F32)
        for j in range(band):
            at = start + z * band + j
            known = jnp.where(mask_s[at] > 0, cutoff_s[at], 1 << 20).astype(F32)
            limit = jnp.where(row == j, known, limit)
        for c in range(depth):
            at = (c * bands + z) * band
            limit_ref[at:at + band] = limit
    facing = jnp.full((1, width), jnp.where(odd, merid_s[band - 1], merid_s[0]), F32)
    for move in moves[5:]:
        move.wait()
    sides = jnp.zeros((band, LANES), F32)
    for k in range(levels):
        v = v_buf[k]
        pair_ref[k:k + 1] = jnp.where(odd, v[:1], v[band - 1:])
        half_ref[k, :2] = jnp.where(odd, p_buf[k, band - 2:], p_buf[k, :2])
        half_ref[k, 2:3] = jnp.where(odd, v[band - 1:], v[:1])
        half_ref[k, 3:4] = facing
        sides = jnp.where(lane == k, pltpu.roll(u_buf[k, :, width - LANES:], (k + 1) % LANES, 1), sides)
        sides = jnp.where(lane == levels + k, pltpu.roll(u_buf[k, :, :LANES], levels + k, 1), sides)
    side_ref[...] = sides


def edges(depth, bands, zonal, merid, level, cutoff, mask, p, u, v):
    levels, band, width = p.shape
    shapes = [(levels + band, width), (levels, 4, width), (band, LANES), (band, LANES), (levels, width), (depth * bands * band, LANES)]
    hbm = pl.BlockSpec(memory_space=pltpu.HBM)
    return pl.pallas_call(
        functools.partial(edges_kernel, depth, bands),
        in_specs=[hbm] * 8,
        out_shape=[jax.ShapeDtypeStruct(shape, F32) for shape in shapes],
        scratch_shapes=[pltpu.SMEM(a.shape, a.dtype) for a in (zonal, merid, level, cutoff, mask)]
        + [pltpu.VMEM(p.shape, F32)] * 3
        + [pltpu.SemaphoreType.DMA((8,))],
        compiler_params=KERNEL,
        cost_estimate=pl.CostEstimate(flops=4 * p.size, bytes_accessed=16 * p.size, transcendentals=0),
        name="edges",
    )(zonal, merid, level, cutoff, mask, p, u, v)


def factor(level_rows, sound, *fields):
    shapes = [sound.shape]
    if fields:
        shapes += [sound.shape]
    return pl.pallas_call(
        factor_kernel,
        in_specs=[pl.BlockSpec(memory_space=pltpu.VMEM)] * (2 + len(fields)),
        out_shape=[jax.ShapeDtypeStruct(shape, F32) for shape in shapes],
        compiler_params=KERNEL,
        cost_estimate=pl.CostEstimate(flops=10 * sound.size, bytes_accessed=16 * sound.size, transcendentals=0),
        name="factor_columns",
    )(level_rows, sound, *fields)


def beside(west_ref, east_ref, k, levels):
    lane = lax.broadcasted_iota(jnp.int32, west_ref.shape, 1)
    west = pltpu.roll(west_ref[...], (LANES - k) % LANES, 1)
    east = pltpu.roll(east_ref[...], LANES - 1 - levels - k, 1)
    return jnp.where(lane == 0, west, jnp.where(lane == LANES - 1, east, 0.0))


def border_weights(own_ref, near, nz, shape, first_step):
    band = shape[0]
    me = lax.axis_index("lat")
    low, high = me == nz // 2 - 1, me == nz // 2
    row = lax.broadcasted_iota(jnp.int32, shape, 0)
    merid = jnp.broadcast_to(own_ref[:, 1:2], shape)
    last, first = merid[band - 1:], merid[:1]
    on_v = jnp.where(low & (row == band - 1), merid, jnp.where(high & (row == 0), -merid, 0.0))
    if not first_step:
        v_first = jnp.where(low & (row == band - 1), merid, 0.0)
        v_second = jnp.where(high & (row == 0), -merid, 0.0)
        return v_first, v_second
    inner = jnp.where(low & (row == band - 2), -merid * last, 0.0)
    outer = jnp.where(low & (row == band - 1), -merid * near, 0.0)
    on_first = jnp.where(high & (row == 0), -merid * near, inner)
    on_second = jnp.where(high & (row == 1), -merid * first, outer)
    on_own = -jnp.where(high & (row == 0), -merid * near, outer)
    return on_first, on_second, on_own, on_v


def sweep(level_ref, sound_ref, inv_ref, w_ref, star, w_out, p_out, finish):
    levels = sound_ref.shape[0]
    here = star(0)
    value = None
    for k in range(levels):
        alpha = level_ref[k:k + 1]
        p_out[k] = here
        if k + 1 < levels:
            upper = star(k + 1)
            rhs = w_ref[k] - alpha * (upper - here)
            here = upper
        else:
            rhs = w_ref[k] + alpha * here
        inv = inv_ref[k]
        scaled = rhs * inv
        value = scaled if value is None else scaled + (alpha * sound_ref[k] * inv) * value
        w_out[k] = value
    upper = w_out[levels - 1]
    for k in range(levels - 1, -1, -1):
        lower = None
        if k:
            lower = w_out[k - 1] + (level_ref[k - 1:k] * sound_ref[k] * inv_ref[k - 1]) * upper
            w_out[k - 1] = lower
        fresh = p_out[k] - sound_ref[k] * (upper if lower is None else upper - lower)
        p_out[k] = fresh
        finish(k, fresh)
        upper = lower


def column_first_kernel(nz, level_ref, own_ref, sound_ref, inv_ref, base_ref, div_ref, p_ref, w_ref, *refs):
    levels, band, width = sound_ref.shape
    per = width // LANES
    if nz:
        edge_ref, pair_ref, west_ref, east_ref, w_out, p_out, sum_out, rows_out = refs
        weights = border_weights(own_ref, edge_ref[0, 3:4], nz, (band, width), True)
        odd = lax.axis_index("lat") % 2 == 1
        row = lax.broadcasted_iota(jnp.int32, (band, width), 0)
        lane = lax.broadcasted_iota(jnp.int32, (band, width), 1)
        zonal, merid = own_ref[:, 0:1], own_ref[:, 1:2]
        on_sides = jnp.where(lane == 0, -zonal, jnp.where(lane == width - 1, zonal, 0.0))
        on_pair = jnp.where(odd & (row == 0), -merid, 0.0)
        on_pair = jnp.where(jnp.logical_not(odd) & (row == band - 1), merid, on_pair)
    else:
        w_out, p_out = refs

    def star(k):
        div = base_ref[k] + div_ref[k]
        if nz:
            div += weights[0] * edge_ref[k, 0:1] + weights[1] * edge_ref[k, 1:2]
            div += weights[2] * p_ref[k] + weights[3] * edge_ref[k, 2:3]
            sides = jnp.concatenate([beside(west_ref, east_ref, k, levels)] * per, axis=1)
            div += on_sides * sides + on_pair * pair_ref[k:k + 1]
        return p_ref[k] - sound_ref[k] * div

    def finish(k, fresh):
        if nz:
            total = p_ref[k] + fresh
            rows_out[k] = jnp.where(odd, total[band - 2:], total[:2])
            sum_out[k] = total

    sweep(level_ref, sound_ref, inv_ref, w_ref, star, w_out, p_out, finish)


def column_last_kernel(nz, level_ref, own_ref, sound_ref, inv_ref, field_ref, p_ref, w_ref, u_ref, v_ref, *refs):
    levels, band, width = sound_ref.shape
    per = width // LANES
    zonal = jnp.broadcast_to(own_ref[:, 0:1], (band, width))
    merid = jnp.broadcast_to(own_ref[:, 1:2], (band, width))
    if nz:
        edge_ref, facing_ref, rows_ref, pair_ref, west_ref, east_ref = refs[:6]
        refs = refs[6:]
        depth = levels // field_ref.shape[0]
        near = edge_ref[0, 3:4]
        weights = border_weights(own_ref, near, nz, (band, width), False)
        odd = lax.axis_index("lat") % 2 == 1
        row = lax.broadcasted_iota(jnp.int32, (band, width), 0)
        lane = lax.broadcasted_iota(jnp.int32, (band, width), 1)
    else:
        base_ref, refs = refs[0], refs[1:]
    u_out, v_out, w_out, p_out = refs[4:8]
    sems = refs[8]
    leaving = []
    size = levels // 4

    def leave(out, start):
        part = pl.ds(start, size)
        move = pltpu.make_async_copy(refs[4 + out].at[part], refs[out].at[part], sems.at[len(leaving)])
        move.start()
        leaving.append(move)

    def wide(k, field):
        at = (field * depth + k % depth) * per * band
        return jnp.concatenate([field_ref[k // depth, at + h * band:at + (h + 1) * band] for h in range(per)], axis=1)

    def star(k):
        result = new_star(k)
        if (k + 1) % size == 0:
            leave(0, k + 1 - size)
            leave(1, k + 1 - size)
        return result

    def finish(k, fresh):
        if k % size == 0:
            leave(2, k)
            leave(3, k)

    def new_star(k):
        if not nz:
            u_out[k] = u_ref[k] - zonal * field_ref[k, band:2 * band]
            v_out[k] = v_ref[k] - merid * field_ref[k, 2 * band:]
            return p_ref[k] - sound_ref[k] * (base_ref[k] + field_ref[k, :band])
        u = u_ref[k] - zonal * wide(k, 0)
        v = v_ref[k] - merid * wide(k, 1)
        far, mine = facing_ref[k], rows_ref[k]
        v -= weights[0] * far[0:1] + weights[1] * far[1:2]
        u_out[k], v_out[k] = u, v
        b, c, at = k // depth, k % depth, 2 * depth * per * band
        sides = unfold(field_ref[b, at + 4:at + 8], c) + beside(west_ref, east_ref, k, levels)
        sides = jnp.concatenate([sides] * per, axis=1)
        at += c * per
        pair = pair_ref[k:k + 1] + jnp.concatenate([field_ref[b, at + h:at + h + 1] for h in range(per)], axis=1)
        half = edge_ref[k, 2:3] - near * jnp.where(odd, far[1:2] - mine[1:2], mine[0:1] - far[0:1])
        north, south = jnp.where(odd, half, pair), jnp.where(odd, pair, half)
        east = jnp.where(lane == width - 1, sides, pltpu.roll(u, width - 1, 1))
        west = jnp.where(lane == 0, sides, pltpu.roll(u, 1, 1))
        up = jnp.where(row == band - 1, north, pltpu.roll(v, band - 1, 0))
        down = jnp.where(row == 0, south, pltpu.roll(v, 1, 0))
        return p_ref[k] - sound_ref[k] * (zonal * (east - west) + merid * (up - down))

    sweep(level_ref, sound_ref, inv_ref, w_ref, star, w_out, p_out, finish)
    for move in leaving:
        move.wait()


def column(first, nz, level_rows, own, sound, *operands):
    levels, _, width = sound.shape
    shapes = [jax.ShapeDtypeStruct(sound.shape, F32)] * (2 if first else 4)
    if first and nz:
        shapes.append(jax.ShapeDtypeStruct(sound.shape, F32))
        shapes.append(jax.ShapeDtypeStruct((levels, 2, width), F32))
    extra = {}
    if not first:
        extra["scratch_shapes"] = [pltpu.VMEM(sound.shape, F32)] * 4 + [pltpu.SemaphoreType.DMA((16,))]
    return pl.pallas_call(
        functools.partial(column_first_kernel if first else column_last_kernel, nz),
        in_specs=[pl.BlockSpec(memory_space=pltpu.VMEM)] * (3 + len(operands)),
        out_specs=[pl.BlockSpec(memory_space=pltpu.VMEM if first else pltpu.HBM)] * len(shapes),
        out_shape=shapes,
        compiler_params=KERNEL,
        cost_estimate=pl.CostEstimate(flops=20 * sound.size, bytes_accessed=40 * sound.size, transcendentals=0),
        name="column_first" if first else "column_last",
        **extra,
    )(level_rows, own, sound, *operands)


def shifted(block, axis, step):
    count = lax.axis_size(axis)
    return lax.ppermute(block, axis, [(i, (i + step) % count) for i in range(count)])


def exchange(block, halves):
    axes, members = "lon", None
    if halves:
        axes = ("lat", "lon")
        count = lax.axis_size(axes)
        members = np.arange(count).reshape(2, count // 2).tolist()
    return lax.all_to_all(block, axes, split_axis=0, concat_axis=0, axis_index_groups=members, tiled=True)


def swapped(block, first):
    count = lax.axis_size("lat")
    pairs = [(i, i + 1) for i in range(first, count - 1, 2)]
    return lax.ppermute(block, "lat", pairs + [(b, a) for a, b in pairs])


def lat_edges(last, first):
    count = lax.axis_size("lat")
    low = lax.ppermute(last, "lat", [(i, i + 1) for i in range(count - 1)])
    high = lax.ppermute(first, "lat", [(i + 1, i) for i in range(count - 1)])
    return low, high


def program(
    zonal_wind,
    merid_wind,
    vertical_wind,
    pressure,
    zonal_coef,
    merid_coef,
    level_coef,
    sound_coef,
    cutoff,
    filter_mask,
):
    levels, band, width = pressure.shape
    nz, nl = lax.axis_size("lat"), lax.axis_size("lon")
    length = width * nl
    lats = band * nz
    me = lax.axis_index("lat")
    weights, table = tables(length)
    level_rows = jnp.broadcast_to(level_coef[:, None], (levels, width))
    own = jnp.stack([zonal_coef, merid_coef], axis=1)
    limit = jnp.where(filter_mask > 0, cutoff, length).astype(F32)
    per = width // LANES

    depth = levels // (2 * nl)
    if nz == 4 and band == 8 and 1 <= depth <= 2 and depth * per <= 4 and levels == 2 * nl * depth and levels <= LANES // 2:
        plan = Plan(True, 2, nl, depth, per, band, 0, band)
        blocks = (levels // depth, depth * band, width)
        circles = exchange(pressure.reshape(blocks), True)
        inputs = (zonal_coef, merid_coef, level_coef, cutoff, filter_mask, pressure, zonal_wind, merid_wind)
        inputs = [pltpu.with_memory_space_constraint(a, pltpu.HBM) for a in inputs]
        pair, half, sides, own, level_rows, limits = edges(depth, 2, *inputs)
        pair = swapped(pair, 0)
        half = swapped(half, 1)
        west, east = shifted(sides, "lon", 1), shifted(sides, "lon", -1)
        inv, base = factor(level_rows, sound_coef, zonal_wind, merid_wind, own)
        div = transform(plan, False, limits, weights, table, circles, own, pair)
        div = exchange(div, True).reshape(levels, band, width)
        w, p, total, rows = column(True, nz, level_rows, own, sound_coef, inv, base, div, pressure, vertical_wind, half, pair, west, east)
        facing = swapped(rows, 1)
        circles = exchange(total.reshape(blocks), True)
        fields = transform(plan, True, limits, weights, table, circles, own, pair)
        fields = exchange(fields, True)
        return column(False, nz, level_rows, own, sound_coef, inv, fields, p, w, zonal_wind, merid_wind, half, facing, rows, pair, west, east)

    depth, halo = levels // nl, 2
    tall = -(-(band + 2 * halo) // 8) * 8
    plan = Plan(False, 1, nl, depth, per, tall, halo, band)

    def spread(field):
        low, high = lat_edges(field[:, -halo:], field[:, :halo])
        field = jnp.concatenate([low, field, high], axis=1)
        field = jnp.pad(field, ((0, 0), (0, tall - band - 2 * halo), (0, 0)))
        return exchange(field.reshape(nl, depth * tall, width), False)

    circles = spread(pressure)
    low, high = lat_edges(own[-halo:], own[:halo])
    v_low, v_high = lat_edges(merid_wind[:, -1:], merid_wind[:, :1])
    row = jnp.arange(lats + 2 * halo) - halo
    limit = jnp.pad(limit, (halo, halo), constant_values=1.0)
    known = jnp.stack([limit, (row < lats - 1).astype(F32), (row > 0).astype(F32)], axis=1)
    known = lax.dynamic_slice_in_dim(known, me * band, band + 2 * halo, 0)
    coefs = jnp.concatenate([known, jnp.concatenate([low, own, high])], axis=1)
    coefs = jnp.tile(jnp.pad(coefs, ((0, tall - band - 2 * halo), (0, 0))), (depth, 1))

    u_low = shifted(zonal_wind[:, :, -1:], "lon", 1)
    u_high = shifted(zonal_wind[:, :, :1], "lon", -1)
    u_diff = jnp.concatenate([zonal_wind[:, :, 1:], u_high], 2) - jnp.concatenate([u_low, zonal_wind[:, :, :-1]], 2)
    v_diff = jnp.concatenate([merid_wind[:, 1:], v_high], 1) - jnp.concatenate([v_low, merid_wind[:, :-1]], 1)
    base = zonal_coef[None, :, None] * u_diff + merid_coef[None, :, None] * v_diff

    (inv,) = factor(level_rows, sound_coef)
    div = transform(plan, False, coefs, weights, table, circles)
    div = exchange(div, False).reshape(levels, band, width)
    w, p = column(True, 0, level_rows, own, sound_coef, inv, base, div, pressure, vertical_wind)
    fields = transform(plan, True, coefs, weights, table, spread(pressure + p))
    fields = exchange(fields, False).reshape(levels, 3 * band, width)
    return column(False, 0, level_rows, own, sound_coef, inv, fields, p, w, zonal_wind, merid_wind, base)


def solution(mesh):
    spec = P(None, "lat", "lon")
    in_specs = (spec, spec, spec, spec, P("lat"), P("lat"), P(), spec, P(), P())
    return jax.shard_map(program, mesh=mesh, in_specs=in_specs, out_specs=(spec,) * 4, check_vma=False)
```

```python
import functools
import math
from typing import NamedTuple

import jax
import jax.numpy as jnp
import numpy as np
from jax import lax
from jax.experimental import pallas as pl
from jax.experimental.pallas import tpu as pltpu
from jax.sharding import PartitionSpec as P


LANES = 128
F32 = jnp.float32
BF16 = jnp.bfloat16
KERNEL = pltpu.CompilerParams(vmem_limit_bytes=8 << 20)


class Plan(NamedTuple):
    packed: bool
    bands: int
    nl: int
    depth: int
    per: int
    tall: int
    skip: int
    band: int

    def fields(self, full):
        if not full:
            return "d"
        return "uv" if self.packed else "duv"


def cmul_const(re, im, cr, ci):
    if im is None:
        return (re * cr if cr != 0.0 else None, re * ci if ci != 0.0 else None)
    return (re * cr - im * ci, re * ci + im * cr)


def add(a, b):
    if a is None:
        return b
    return a if b is None else a + b


def sub(a, b):
    if b is None:
        return a
    return -b if a is None else a - b


def neg(a):
    return None if a is None else -a


def unit(num, den):
    turn = num % den
    table = {0: (1.0, 0.0), den / 4: (0.0, 1.0), den / 2: (-1.0, 0.0), 3 * den / 4: (0.0, -1.0)}
    if turn in table:
        return table[turn]
    angle = 2.0 * math.pi * turn / den
    return math.cos(angle), math.sin(angle)


def rotate(z, num, den):
    cr, ci = unit(num, den)
    re, im = z
    if (cr, ci) == (1.0, 0.0):
        return z
    if (cr, ci) == (0.0, 1.0):
        return (neg(im), re)
    if (cr, ci) == (0.0, -1.0):
        return (im, neg(re))
    return cmul_const(re, im, cr, ci)


def real_dft(pieces):
    n = len(pieces)
    if n == 1:
        return [(pieces[0], None)]
    even, odd = real_dft(pieces[0::2]), real_dft(pieces[1::2])
    out = [None] * (n // 2 + 1)
    for s in range(n // 4 + 1 if n > 2 else 1):
        er, ei = even[s]
        tr, ti = rotate(odd[s], -s, n)
        out[n // 2 - s] = (sub(er, tr), sub(ti, ei))
        out[s] = (add(er, tr), add(ei, ti))
    return out


def real_dft_inverse(groups):
    n = 2 * (len(groups) - 1)
    if n == 0:
        return [groups[0][0]]
    if n == 2:
        a, b = groups[0][0], groups[1][0]
        return [a + b, a - b]
    even, odd = [], []
    for s in range(n // 4 + 1):
        ar, ai = groups[s]
        br, bi = groups[n // 2 - s]
        even.append((add(ar, br), sub(ai, bi)))
        odd.append(rotate((sub(ar, br), add(ai, bi)), s, n))
    even[0] = (even[0][0], None)
    odd[0] = (odd[0][0], None)
    even[-1] = (even[-1][0], None)
    odd[-1] = (odd[-1][0], None)
    out = [None] * n
    out[0::2] = real_dft_inverse(even)
    out[1::2] = real_dft_inverse(odd)
    return out


def tables(length):
    pieces = length // LANES
    groups = pieces // 2 + 1
    lane = np.arange(LANES)
    angle = 2.0 * np.pi / LANES * (np.outer(lane, lane) % LANES)
    cos, sin = np.cos(angle), np.sin(angle)
    matrix = np.block([[cos, -sin], [sin, cos]])

    def halves(m):
        m = m.astype(np.float32)
        high = m.astype(BF16)
        return np.stack([high, (m - high.astype(np.float32)).astype(BF16)])

    weights = np.stack([halves(matrix), halves(matrix.T)])
    s = np.arange(groups)[:, None]
    turn = 2.0 * np.pi / length * (s * lane[None, :])
    wavenum = pieces * lane[None, :] + s
    wavenum = np.minimum(wavenum, length - wavenum).astype(np.float64)
    slope = 2.0 * np.sin(2.0 * np.pi / length * (pieces * lane[None, :] + s))
    rows = np.stack([np.cos(turn), np.sin(turn), wavenum, 1.0 / np.maximum(wavenum, 1.0) ** 2, slope])
    return weights, rows.astype(np.float32)


def matmul(weight_ref, lhs_ref, size, rows):
    def product(which, start):
        high, low = (lhs_ref[i, start:start + size] for i in range(2))
        total = jnp.dot(high, weight_ref[which, 0], preferred_element_type=F32)
        total += jnp.dot(low, weight_ref[which, 0], preferred_element_type=F32)
        return total + jnp.dot(high, weight_ref[which, 1], preferred_element_type=F32)

    def put(row, re, im):
        for half, part in enumerate((re, im)):
            high = part.astype(BF16)
            low = (part - high.astype(F32)).astype(BF16)
            lhs_ref[0, row:row + rows, half * LANES:(half + 1) * LANES] = high
            lhs_ref[1, row:row + rows, half * LANES:(half + 1) * LANES] = low

    return product, put


def forward(plan, x_ref, weight_ref, table_ref, spec_ref, lhs_ref):
    bands, nl, depth, per, tall = plan.bands, plan.nl, plan.depth, plan.per, plan.tall
    rows = depth * bands * tall
    groups = nl * per // 2 + 1
    product, put = matmul(weight_ref, lhs_ref, groups * rows, rows)

    def tile(c, z, l, h):
        return x_ref[z * nl + l, c * tall:(c + 1) * tall, h * LANES:(h + 1) * LANES]

    chunks = []
    for l in range(nl):
        for h in range(per):
            chunks.append(jnp.concatenate([tile(c, z, l, h) for c in range(depth) for z in range(bands)], axis=0))
    zero = jnp.zeros((rows, LANES), F32)
    for s, (re, im) in enumerate(real_dft(chunks)):
        if s:
            cr, ci = table_ref[0, s:s + 1], table_ref[1, s:s + 1]
            if im is None:
                re, im = re * cr, -re * ci
            else:
                re, im = re * cr + im * ci, im * cr - re * ci
        put(s * rows, re, zero if im is None else im)
    spec_ref[...] = product(0, 0)


def spectra_of(plan, x, weights, table):
    size = table.shape[1] * plan.depth * plan.bands * plan.tall
    return pl.pallas_call(
        functools.partial(forward, plan),
        out_shape=jax.ShapeDtypeStruct((size, 2 * LANES), F32),
        scratch_shapes=[pltpu.VMEM((2, size, 2 * LANES), BF16)],
        compiler_params=KERNEL,
        cost_estimate=pl.CostEstimate(flops=3 * 2 * 65536 * size, bytes_accessed=8 * x.size, transcendentals=0),
        name="transform_forward",
    )(x, weights, table)


def transform_kernel(plan, full, x_ref, *refs):
    if plan.packed:
        own_ref, near_ref, refs = refs[0], refs[1], refs[2:]
    coef_ref, weight_ref, table_ref, result_ref, lhs_ref, spec_ref, work_ref, out_ref, sems = refs
    bands, nl, depth, per = plan.bands, plan.nl, plan.depth, plan.per
    tall, skip, band = plan.tall, plan.skip, plan.band
    stacks = depth * bands
    pieces = nl * per
    groups = pieces // 2 + 1
    rows = stacks * tall
    length = pieces * LANES

    if len(x_ref.shape) == 3:
        forward(plan, x_ref, weight_ref, table_ref, spec_ref, lhs_ref)
    else:
        spec_ref = x_ref
    product, put = matmul(weight_ref, lhs_ref, groups * rows, rows)

    def column(a):
        return jnp.broadcast_to(a, (a.shape[0], LANES))

    if plan.packed:
        limit = coef_ref[...]
        place = lax.broadcasted_iota(jnp.int32, (rows, LANES), 0) % (bands * tall)
        has_up = jnp.where(place < bands * tall - 1, 1.0, 0.0)
        has_down = jnp.where(place > 0, 1.0, 0.0)
        odd = lax.axis_index("lat") % 2 == 1
        own_rows, near_rows = own_ref[...], near_ref[-tall:, :LANES]
        pair = [jnp.where(odd, near_rows, own_rows), jnp.where(odd, own_rows, near_rows)]
        zonal = jnp.concatenate([column(t[:, 0:1]) for t in pair] * depth, axis=0)
        merid = jnp.concatenate([column(t[:, 1:2]) for t in pair] * depth, axis=0)
    else:
        limit, has_up, has_down, zonal, merid = (column(coef_ref[:, i:i + 1]) for i in range(5))
    zonal2, merid_up, merid_down = zonal * zonal, merid * has_up, merid * has_down
    limit2 = limit * limit

    def above(a):
        return pltpu.roll(a, rows - 1, 0)

    def below(a):
        return pltpu.roll(a, 1, 0)

    for s in range(groups):
        wavenum, inverse2, slope = (table_ref[i, s:s + 1] for i in (2, 3, 4))
        factor = jnp.where(wavenum > limit, limit2 * inverse2, 1.0)
        parts = [spec_ref[s * rows:(s + 1) * rows, half * LANES:(half + 1) * LANES] for half in (0, 1)]
        spread2 = zonal2 * (slope * slope)
        filtered = [factor * part for part in parts]
        merids, divs = [], []
        for part, filt in zip(parts, filtered):
            across = factor * (has_up * above(part) - has_down * below(part))
            flux = merid * across
            merids.append(across)
            divs.append(spread2 * filt - merid_up * above(flux) + merid_down * below(flux))
        spectra = {"d": divs, "u": (-slope * filtered[1], slope * filtered[0]), "v": merids}
        for field, name in enumerate(plan.fields(full)):
            put((field * groups + s) * rows, *spectra[name])

    row = lax.broadcasted_iota(jnp.int32, (band, LANES), 0)
    lane = lax.broadcasted_iota(jnp.int32, (band, LANES), 1)
    cells = [(c, z, l) for c in range(depth) for z in range(bands) for l in range(nl)]

    def latitudes(c, z):
        first = (c * bands + z) * tall + skip
        return slice(first, first + band)

    leaving = []

    def leave(start, size):
        part = (slice(None), pl.ds(start, size))
        move = pltpu.make_async_copy(out_ref.at[part], result_ref.at[part], sems.at[len(leaving)])
        move.start()
        leaving.append(move)

    results = []
    for field in range(len(plan.fields(full))):
        base = field * groups * rows
        work_ref[...] = product(1, base)
        spectrum = []
        for s in range(groups):
            re = work_ref[s * rows:(s + 1) * rows, :LANES]
            im = work_ref[s * rows:(s + 1) * rows, LANES:]
            if s:
                cr, ci = table_ref[0, s:s + 1], table_ref[1, s:s + 1]
                re, im = re * cr - im * ci, (None if s == groups - 1 else re * ci + im * cr)
            else:
                im = None
            spectrum.append((re, im))
        result = [piece * (1.0 / length) for piece in real_dft_inverse(spectrum)]
        results.append(result)
        for c, z, l in cells:
            own = latitudes(c, z)
            for h in range(per):
                value = result[l * per + h][own]
                if plan.packed and full:
                    start = ((field * depth + c) * per + h) * band
                    out_ref[z * nl + l, start:start + band] = value
                    continue
                start = (c * len(plan.fields(full)) + field) * band
                out_ref[z * nl + l, start:start + band, h * LANES:(h + 1) * LANES] = value
        if plan.packed and full:
            leave(field * depth * per * band, depth * per * band)
    if plan.packed and full:
        u, v = results
        base = 2 * depth * per * band
        for z in range(bands):
            for l in range(nl):
                edge = None
                for c in range(depth):
                    own = latitudes(c, z)
                    before = u[(l * per - 1) % pieces][own]
                    after = u[(l * per + per) % pieces][own]
                    before = -zonal[own] * pltpu.roll(before, 1, 1)
                    after = -zonal[own] * pltpu.roll(after, LANES - 1, 1)
                    sides = jnp.where(lane == 0, before, jnp.where(lane == LANES - 1, after, 0.0))
                    edge = sides if c == 0 else edge + pltpu.roll(sides, c * (LANES // 4), 1)
                    other = latitudes(c, z ^ 1)
                    other = other.start if z % 2 == 0 else other.stop - 1
                    at = c * per
                    for h in range(per):
                        moved = merid[other:other + 1] * v[l * per + h][other:other + 1]
                        out_ref[z * nl + l, base + at + h:base + at + h + 1] = -moved
                out_ref[z * nl + l, base + 4:base + 8] = fold(edge, row)
                if depth * per < 4:
                    out_ref[z * nl + l, base + depth * per:base + 4] = jnp.zeros((4 - depth * per, LANES), F32)
        leave(base, 8)
    else:
        leave(0, out_ref.shape[1])
    for move in leaving:
        move.wait()


def fold(edge, row):
    edge = jnp.where(row < 4, edge, pltpu.roll(edge, LANES // 2, 1))
    return edge[:4] + edge[4:]


def unfold(part, c):
    tile = jnp.concatenate([part, pltpu.roll(part, LANES // 2, 1)], axis=0)
    return pltpu.roll(tile, LANES - c * (LANES // 4), 1) if c else tile


def transform(plan, full, coefs, weights, table, *operands):
    rows = plan.depth * plan.bands * plan.tall
    fields = len(plan.fields(full))
    groups = table.shape[1]
    count = fields * groups * rows
    blocks, width = plan.bands * plan.nl, plan.per * LANES
    shape = (blocks, plan.depth * fields * plan.band, width)
    if plan.packed and full:
        shape = (blocks, (2 * plan.depth * plan.per + 1) * plan.band, LANES)
    return pl.pallas_call(
        functools.partial(transform_kernel, plan, full),
        out_specs=pl.BlockSpec(memory_space=pltpu.HBM),
        out_shape=jax.ShapeDtypeStruct(shape, F32),
        scratch_shapes=[
            pltpu.VMEM((2, count, 2 * LANES), BF16),
            pltpu.VMEM((groups * rows, 2 * LANES), F32),
            pltpu.VMEM((groups * rows, 2 * LANES), F32),
            pltpu.VMEM(shape, F32),
            pltpu.SemaphoreType.DMA((3,)),
        ],
        compiler_params=KERNEL,
        cost_estimate=pl.CostEstimate(flops=6 * 2 * 65536 * count, bytes_accessed=32 * blocks * plan.depth * plan.band * width, transcendentals=0),
        name="transform_all" if full else "transform_div",
    )(*operands, coefs, weights, table)


def factor_kernel(level_ref, sound_ref, *refs):
    levels, band, width = sound_ref.shape
    full = len(refs) > 1
    if full:
        u_ref, v_ref, own_ref, inv_ref, base_ref = refs
        row = lax.broadcasted_iota(jnp.int32, (band, width), 0)
        lane = lax.broadcasted_iota(jnp.int32, (band, width), 1)
        zonal, merid = own_ref[:, 0:1], own_ref[:, 1:2]
        east = jnp.where(lane < width - 1, zonal, 0.0)
        west = jnp.where(lane > 0, zonal, 0.0)
        north = jnp.where(row < band - 1, merid, 0.0)
        south = jnp.where(row > 0, merid, 0.0)
    else:
        (inv_ref,) = refs
    prev = jnp.zeros((band, width), F32)
    for k in range(levels):
        alpha = level_ref[k:k + 1]
        below = alpha * sound_ref[k]
        above = alpha * sound_ref[k + 1] if k + 1 < levels else jnp.zeros_like(below)
        inv = 1.0 / (1.0 + below + above + below * prev)
        prev = -above * inv
        inv_ref[k] = inv
        if full:
            u, v = u_ref[k], v_ref[k]
            div = east * pltpu.roll(u, width - 1, 1) - west * pltpu.roll(u, 1, 1)
            base_ref[k] = div + north * pltpu.roll(v, band - 1, 0) - south * pltpu.roll(v, 1, 0)


def edges_kernel(depth, bands, zonal_ref, merid_ref, level_ref, cutoff_ref, mask_ref, p_ref, u_ref, v_ref, *refs):
    pair_ref, half_ref, side_ref, own_ref, rows_ref, limit_ref = refs[:6]
    smalls, (p_buf, u_buf, v_buf), sems = refs[6:11], refs[11:14], refs[14]
    levels, band, width = u_buf.shape
    moves = []
    for source, target in zip((zonal_ref, merid_ref, level_ref, cutoff_ref, mask_ref, p_ref, u_ref, v_ref), (*smalls, p_buf, u_buf, v_buf)):
        moves.append(pltpu.make_async_copy(source, target, sems.at[len(moves)]))
        moves[-1].start()
    for move in moves[:5]:
        move.wait()
    zonal_s, merid_s, level_s, cutoff_s, mask_s = smalls
    me = lax.axis_index("lat")
    odd = me % 2 == 1
    row = lax.broadcasted_iota(jnp.int32, (band, LANES), 0)
    lane = lax.broadcasted_iota(jnp.int32, (band, LANES), 1)
    own = jnp.zeros((band, LANES), F32)
    for j in range(band):
        own = jnp.where(row == j, jnp.where(lane == 0, zonal_s[j], jnp.where(lane == 1, merid_s[j], 0.0)), own)
    own_ref[...] = own
    pair_ref[levels:, :LANES] = own
    if width > LANES:
        pair_ref[levels:, LANES:] = jnp.zeros((band, width - LANES), F32)
    for k in range(levels):
        rows_ref[k:k + 1] = jnp.full((1, width), level_s[k], F32)
    start = me // bands * bands * band
    for z in range(bands):
        limit = jnp.zeros((band, LANES), F32)
        for j in range(band):
            at = start + z * band + j
            known = jnp.where(mask_s[at] > 0, cutoff_s[at], 1 << 20).astype(F32)
            limit = jnp.where(row == j, known, limit)
        for c in range(depth):
            at = (c * bands + z) * band
            limit_ref[at:at + band] = limit
    facing = jnp.full((1, width), jnp.where(odd, merid_s[band - 1], merid_s[0]), F32)
    for move in moves[5:]:
        move.wait()
    sides = jnp.zeros((band, LANES), F32)
    for k in range(levels):
        v = v_buf[k]
        pair_ref[k:k + 1] = jnp.where(odd, v[:1], v[band - 1:])
        half_ref[k, :2] = jnp.where(odd, p_buf[k, band - 2:], p_buf[k, :2])
        half_ref[k, 2:3] = jnp.where(odd, v[band - 1:], v[:1])
        half_ref[k, 3:4] = facing
        sides = jnp.where(lane == k, pltpu.roll(u_buf[k, :, width - LANES:], (k + 1) % LANES, 1), sides)
        sides = jnp.where(lane == levels + k, pltpu.roll(u_buf[k, :, :LANES], levels + k, 1), sides)
    side_ref[...] = sides


def edges(depth, bands, zonal, merid, level, cutoff, mask, p, u, v):
    levels, band, width = p.shape
    shapes = [(levels + band, width), (levels, 4, width), (band, LANES), (band, LANES), (levels, width), (depth * bands * band, LANES)]
    hbm = pl.BlockSpec(memory_space=pltpu.HBM)
    return pl.pallas_call(
        functools.partial(edges_kernel, depth, bands),
        in_specs=[hbm] * 8,
        out_shape=[jax.ShapeDtypeStruct(shape, F32) for shape in shapes],
        scratch_shapes=[pltpu.SMEM(a.shape, a.dtype) for a in (zonal, merid, level, cutoff, mask)]
        + [pltpu.VMEM(p.shape, F32)] * 3
        + [pltpu.SemaphoreType.DMA((8,))],
        compiler_params=KERNEL,
        cost_estimate=pl.CostEstimate(flops=4 * p.size, bytes_accessed=16 * p.size, transcendentals=0),
        name="edges",
    )(zonal, merid, level, cutoff, mask, p, u, v)


def factor(level_rows, sound, *fields):
    shapes = [sound.shape]
    if fields:
        shapes += [sound.shape]
    return pl.pallas_call(
        factor_kernel,
        in_specs=[pl.BlockSpec(memory_space=pltpu.VMEM)] * (2 + len(fields)),
        out_shape=[jax.ShapeDtypeStruct(shape, F32) for shape in shapes],
        compiler_params=KERNEL,
        cost_estimate=pl.CostEstimate(flops=10 * sound.size, bytes_accessed=16 * sound.size, transcendentals=0),
        name="factor_columns",
    )(level_rows, sound, *fields)


def beside(west_ref, east_ref, k, levels):
    lane = lax.broadcasted_iota(jnp.int32, west_ref.shape, 1)
    west = pltpu.roll(west_ref[...], (LANES - k) % LANES, 1)
    east = pltpu.roll(east_ref[...], LANES - 1 - levels - k, 1)
    return jnp.where(lane == 0, west, jnp.where(lane == LANES - 1, east, 0.0))


def border_weights(own_ref, near, nz, shape, first_step):
    band = shape[0]
    me = lax.axis_index("lat")
    low, high = me == nz // 2 - 1, me == nz // 2
    row = lax.broadcasted_iota(jnp.int32, shape, 0)
    merid = jnp.broadcast_to(own_ref[:, 1:2], shape)
    last, first = merid[band - 1:], merid[:1]
    on_v = jnp.where(low & (row == band - 1), merid, jnp.where(high & (row == 0), -merid, 0.0))
    if not first_step:
        v_first = jnp.where(low & (row == band - 1), merid, 0.0)
        v_second = jnp.where(high & (row == 0), -merid, 0.0)
        return v_first, v_second
    inner = jnp.where(low & (row == band - 2), -merid * last, 0.0)
    outer = jnp.where(low & (row == band - 1), -merid * near, 0.0)
    on_first = jnp.where(high & (row == 0), -merid * near, inner)
    on_second = jnp.where(high & (row == 1), -merid * first, outer)
    on_own = -jnp.where(high & (row == 0), -merid * near, outer)
    return on_first, on_second, on_own, on_v


def sweep(level_ref, sound_ref, inv_ref, w_ref, star, w_out, p_out, finish):
    levels = sound_ref.shape[0]
    here = star(0)
    value = None
    for k in range(levels):
        alpha = level_ref[k:k + 1]
        p_out[k] = here
        if k + 1 < levels:
            upper = star(k + 1)
            rhs = w_ref[k] - alpha * (upper - here)
            here = upper
        else:
            rhs = w_ref[k] + alpha * here
        inv = inv_ref[k]
        scaled = rhs * inv
        value = scaled if value is None else scaled + (alpha * sound_ref[k] * inv) * value
        w_out[k] = value
    upper = w_out[levels - 1]
    for k in range(levels - 1, -1, -1):
        lower = None
        if k:
            lower = w_out[k - 1] + (level_ref[k - 1:k] * sound_ref[k] * inv_ref[k - 1]) * upper
            w_out[k - 1] = lower
        fresh = p_out[k] - sound_ref[k] * (upper if lower is None else upper - lower)
        p_out[k] = fresh
        finish(k, fresh)
        upper = lower


def column_first_kernel(nz, level_ref, own_ref, sound_ref, inv_ref, base_ref, div_ref, p_ref, w_ref, *refs):
    levels, band, width = sound_ref.shape
    per = width // LANES
    if nz:
        edge_ref, pair_ref, west_ref, east_ref, w_out, p_out, sum_out, rows_out = refs
        weights = border_weights(own_ref, edge_ref[0, 3:4], nz, (band, width), True)
        odd = lax.axis_index("lat") % 2 == 1
        row = lax.broadcasted_iota(jnp.int32, (band, width), 0)
        lane = lax.broadcasted_iota(jnp.int32, (band, width), 1)
        zonal, merid = own_ref[:, 0:1], own_ref[:, 1:2]
        on_sides = jnp.where(lane == 0, -zonal, jnp.where(lane == width - 1, zonal, 0.0))
        on_pair = jnp.where(odd & (row == 0), -merid, 0.0)
        on_pair = jnp.where(jnp.logical_not(odd) & (row == band - 1), merid, on_pair)
    else:
        w_out, p_out = refs

    def star(k):
        div = base_ref[k] + div_ref[k]
        if nz:
            div += weights[0] * edge_ref[k, 0:1] + weights[1] * edge_ref[k, 1:2]
            div += weights[2] * p_ref[k] + weights[3] * edge_ref[k, 2:3]
            sides = jnp.concatenate([beside(west_ref, east_ref, k, levels)] * per, axis=1)
            div += on_sides * sides + on_pair * pair_ref[k:k + 1]
        return p_ref[k] - sound_ref[k] * div

    def finish(k, fresh):
        if nz:
            total = p_ref[k] + fresh
            rows_out[k] = jnp.where(odd, total[band - 2:], total[:2])
            sum_out[k] = total

    sweep(level_ref, sound_ref, inv_ref, w_ref, star, w_out, p_out, finish)


def column_last_kernel(nz, level_ref, own_ref, sound_ref, inv_ref, field_ref, p_ref, w_ref, u_ref, v_ref, *refs):
    levels, band, width = sound_ref.shape
    per = width // LANES
    zonal = jnp.broadcast_to(own_ref[:, 0:1], (band, width))
    merid = jnp.broadcast_to(own_ref[:, 1:2], (band, width))
    if nz:
        edge_ref, facing_ref, rows_ref, pair_ref, west_ref, east_ref = refs[:6]
        refs = refs[6:]
        depth = levels // field_ref.shape[0]
        near = edge_ref[0, 3:4]
        weights = border_weights(own_ref, near, nz, (band, width), False)
        odd = lax.axis_index("lat") % 2 == 1
        row = lax.broadcasted_iota(jnp.int32, (band, width), 0)
        lane = lax.broadcasted_iota(jnp.int32, (band, width), 1)
    else:
        base_ref, refs = refs[0], refs[1:]
    u_out, v_out, w_out, p_out = refs[4:8]
    sems = refs[8]
    leaving = []
    size = levels // 8

    def leave(out, start):
        part = pl.ds(start, size)
        move = pltpu.make_async_copy(refs[4 + out].at[part], refs[out].at[part], sems.at[len(leaving)])
        move.start()
        leaving.append(move)

    def wide(k, field):
        at = (field * depth + k % depth) * per * band
        return jnp.concatenate([field_ref[k // depth, at + h * band:at + (h + 1) * band] for h in range(per)], axis=1)

    def star(k):
        result = new_star(k)
        if (k + 1) % size == 0:
            leave(0, k + 1 - size)
            leave(1, k + 1 - size)
        return result

    def finish(k, fresh):
        if k % size == 0:
            leave(2, k)
            leave(3, k)

    def new_star(k):
        if not nz:
            u_out[k] = u_ref[k] - zonal * field_ref[k, band:2 * band]
            v_out[k] = v_ref[k] - merid * field_ref[k, 2 * band:]
            return p_ref[k] - sound_ref[k] * (base_ref[k] + field_ref[k, :band])
        u = u_ref[k] - zonal * wide(k, 0)
        v = v_ref[k] - merid * wide(k, 1)
        far, mine = facing_ref[k], rows_ref[k]
        v -= weights[0] * far[0:1] + weights[1] * far[1:2]
        u_out[k], v_out[k] = u, v
        b, c, at = k // depth, k % depth, 2 * depth * per * band
        sides = unfold(field_ref[b, at + 4:at + 8], c) + beside(west_ref, east_ref, k, levels)
        sides = jnp.concatenate([sides] * per, axis=1)
        at += c * per
        pair = pair_ref[k:k + 1] + jnp.concatenate([field_ref[b, at + h:at + h + 1] for h in range(per)], axis=1)
        half = edge_ref[k, 2:3] - near * jnp.where(odd, far[1:2] - mine[1:2], mine[0:1] - far[0:1])
        north, south = jnp.where(odd, half, pair), jnp.where(odd, pair, half)
        east = jnp.where(lane == width - 1, sides, pltpu.roll(u, width - 1, 1))
        west = jnp.where(lane == 0, sides, pltpu.roll(u, 1, 1))
        up = jnp.where(row == band - 1, north, pltpu.roll(v, band - 1, 0))
        down = jnp.where(row == 0, south, pltpu.roll(v, 1, 0))
        return p_ref[k] - sound_ref[k] * (zonal * (east - west) + merid * (up - down))

    sweep(level_ref, sound_ref, inv_ref, w_ref, star, w_out, p_out, finish)
    for move in leaving:
        move.wait()


def column(first, nz, level_rows, own, sound, *operands):
    levels, _, width = sound.shape
    shapes = [jax.ShapeDtypeStruct(sound.shape, F32)] * (2 if first else 4)
    if first and nz:
        shapes.append(jax.ShapeDtypeStruct(sound.shape, F32))
        shapes.append(jax.ShapeDtypeStruct((levels, 2, width), F32))
    extra = {}
    if not first:
        extra["scratch_shapes"] = [pltpu.VMEM(sound.shape, F32)] * 4 + [pltpu.SemaphoreType.DMA((32,))]
    return pl.pallas_call(
        functools.partial(column_first_kernel if first else column_last_kernel, nz),
        in_specs=[pl.BlockSpec(memory_space=pltpu.VMEM)] * (3 + len(operands)),
        out_specs=[pl.BlockSpec(memory_space=pltpu.VMEM if first else pltpu.HBM)] * len(shapes),
        out_shape=shapes,
        compiler_params=KERNEL,
        cost_estimate=pl.CostEstimate(flops=20 * sound.size, bytes_accessed=40 * sound.size, transcendentals=0),
        name="column_first" if first else "column_last",
        **extra,
    )(level_rows, own, sound, *operands)


def shifted(block, axis, step):
    count = lax.axis_size(axis)
    return lax.ppermute(block, axis, [(i, (i + step) % count) for i in range(count)])


def exchange(block, halves):
    axes, members = "lon", None
    if halves:
        axes = ("lat", "lon")
        count = lax.axis_size(axes)
        members = np.arange(count).reshape(2, count // 2).tolist()
    return lax.all_to_all(block, axes, split_axis=0, concat_axis=0, axis_index_groups=members, tiled=True)


def swapped(block, first):
    count = lax.axis_size("lat")
    pairs = [(i, i + 1) for i in range(first, count - 1, 2)]
    return lax.ppermute(block, "lat", pairs + [(b, a) for a, b in pairs])


def lat_edges(last, first):
    count = lax.axis_size("lat")
    low = lax.ppermute(last, "lat", [(i, i + 1) for i in range(count - 1)])
    high = lax.ppermute(first, "lat", [(i + 1, i) for i in range(count - 1)])
    return low, high


def program(
    zonal_wind,
    merid_wind,
    vertical_wind,
    pressure,
    zonal_coef,
    merid_coef,
    level_coef,
    sound_coef,
    cutoff,
    filter_mask,
):
    levels, band, width = pressure.shape
    nz, nl = lax.axis_size("lat"), lax.axis_size("lon")
    length = width * nl
    lats = band * nz
    me = lax.axis_index("lat")
    weights, table = tables(length)
    level_rows = jnp.broadcast_to(level_coef[:, None], (levels, width))
    own = jnp.stack([zonal_coef, merid_coef], axis=1)
    limit = jnp.where(filter_mask > 0, cutoff, length).astype(F32)
    per = width // LANES

    depth = levels // (2 * nl)
    if nz == 4 and band == 8 and 1 <= depth <= 2 and depth * per <= 4 and levels == 2 * nl * depth and levels <= LANES // 2:
        plan = Plan(True, 2, nl, depth, per, band, 0, band)
        blocks = (levels // depth, depth * band, width)
        circles = exchange(pressure.reshape(blocks), True)
        inputs = (zonal_coef, merid_coef, level_coef, cutoff, filter_mask, pressure, zonal_wind, merid_wind)
        inputs = [pltpu.with_memory_space_constraint(a, pltpu.HBM) for a in inputs]
        pair, half, sides, own, level_rows, limits = edges(depth, 2, *inputs)
        pair = swapped(pair, 0)
        half = swapped(half, 1)
        west, east = shifted(sides, "lon", 1), shifted(sides, "lon", -1)
        inv, base = factor(level_rows, sound_coef, zonal_wind, merid_wind, own)
        circles = spectra_of(plan, circles, weights, table)
        div = transform(plan, False, limits, weights, table, circles, own, pair)
        div = exchange(div, True).reshape(levels, band, width)
        w, p, total, rows = column(True, nz, level_rows, own, sound_coef, inv, base, div, pressure, vertical_wind, half, pair, west, east)
        facing = swapped(rows, 1)
        circles = exchange(total.reshape(blocks), True)
        fields = transform(plan, True, limits, weights, table, circles, own, pair)
        fields = exchange(fields, True)
        return column(False, nz, level_rows, own, sound_coef, inv, fields, p, w, zonal_wind, merid_wind, half, facing, rows, pair, west, east)

    depth, halo = levels // nl, 2
    tall = -(-(band + 2 * halo) // 8) * 8
    plan = Plan(False, 1, nl, depth, per, tall, halo, band)

    def spread(field):
        low, high = lat_edges(field[:, -halo:], field[:, :halo])
        field = jnp.concatenate([low, field, high], axis=1)
        field = jnp.pad(field, ((0, 0), (0, tall - band - 2 * halo), (0, 0)))
        return exchange(field.reshape(nl, depth * tall, width), False)

    circles = spread(pressure)
    low, high = lat_edges(own[-halo:], own[:halo])
    v_low, v_high = lat_edges(merid_wind[:, -1:], merid_wind[:, :1])
    row = jnp.arange(lats + 2 * halo) - halo
    limit = jnp.pad(limit, (halo, halo), constant_values=1.0)
    known = jnp.stack([limit, (row < lats - 1).astype(F32), (row > 0).astype(F32)], axis=1)
    known = lax.dynamic_slice_in_dim(known, me * band, band + 2 * halo, 0)
    coefs = jnp.concatenate([known, jnp.concatenate([low, own, high])], axis=1)
    coefs = jnp.tile(jnp.pad(coefs, ((0, tall - band - 2 * halo), (0, 0))), (depth, 1))

    u_low = shifted(zonal_wind[:, :, -1:], "lon", 1)
    u_high = shifted(zonal_wind[:, :, :1], "lon", -1)
    u_diff = jnp.concatenate([zonal_wind[:, :, 1:], u_high], 2) - jnp.concatenate([u_low, zonal_wind[:, :, :-1]], 2)
    v_diff = jnp.concatenate([merid_wind[:, 1:], v_high], 1) - jnp.concatenate([v_low, merid_wind[:, :-1]], 1)
    base = zonal_coef[None, :, None] * u_diff + merid_coef[None, :, None] * v_diff

    (inv,) = factor(level_rows, sound_coef)
    div = transform(plan, False, coefs, weights, table, circles)
    div = exchange(div, False).reshape(levels, band, width)
    w, p = column(True, 0, level_rows, own, sound_coef, inv, base, div, pressure, vertical_wind)
    fields = transform(plan, True, coefs, weights, table, spread(pressure + p))
    fields = exchange(fields, False).reshape(levels, 3 * band, width)
    return column(False, 0, level_rows, own, sound_coef, inv, fields, p, w, zonal_wind, merid_wind, base)


def solution(mesh):
    spec = P(None, "lat", "lon")
    in_specs = (spec, spec, spec, spec, P("lat"), P("lat"), P(), spec, P(), P())
    return jax.shard_map(program, mesh=mesh, in_specs=in_specs, out_specs=(spec,) * 4, check_vma=False)
```
